32 devices in a mesh: groups: 2 (over x), tile: 16 (over z, y, core).
Axes of the slice: x: 2, y: 2, z: 4, core: 2. Of those that a mesh axis runs over, the one named last changes fastest.
Arguments:
- features: bfloat16 [8, 384, 16, 8, 16], P('groups', None, 'tile'), parts along dimension 0, may hold values from -6 to 6
- cache_first: bfloat16 [4, 384, 16, 8, 16], P('groups', None, 'tile'), parts along dimension 0, may hold values from -6 to 6
- cache_second: bfloat16 [4, 192, 16, 16, 32], P('groups', None, 'tile'), parts along dimension 0, may hold values from -6 to 6
- cache_third: bfloat16 [4, 96, 16, 32, 64], P('groups', None, 'tile'), parts along dimension 0, may hold values from -6 to 6
- weight_first: bfloat16 [3, 3, 3, 192, 384], replicated, may hold values from -0.0625 to 0.0625
- weight_second: bfloat16 [3, 3, 3, 96, 192], replicated, may hold values from -0.078125 to 0.078125
- weight_third: bfloat16 [3, 3, 3, 3, 96], replicated, may hold values from -0.125 to 0.125
- gain_first: float32 [384], replicated, may hold values from 0.1 to 1.9
- gain_second: float32 [192], replicated, may hold values from 0.1 to 1.9
- gain_third: float32 [96], replicated, may hold values from 0.1 to 1.9
Outputs:
- pixels: float32 [8, 3, 16, 32, 64], P('groups', None, 'tile'), parts along dimension 0
The draws below stay inside these ranges and needn't reach their ends.
There are 2 independent parts, one for each index of `groups`. The reference program is written for one: setup_inputs(seed, part) draws one part's arguments, and reference() takes and returns one part's arrays. A program takes and returns all parts, laid end to end along the dimension named above; an argument that names none is the same for every part. Nothing has to cross between parts.
All inputs are finite; a program needn't handle non-finite values.
Results may differ from the reference program's by a relative error of at most 0.0085.
Values may be sent and summed in bfloat16 or wider, within the bound.
No kernel may reach another device: no remote copies, remote signals or barrier semaphores. Data moves between devices by JAX's collectives and lax.ppermute only.
A program may use at most 64 MiB of HBM per device.

```python
import jax
import jax.numpy as jnp
from jax import lax

C1 = 384
C2 = 192
C3 = 96
RGB = 3
TILES_X = 8
TILE_H = 8
TILE_W = 16
FRAMES = 4
N_TILE = 16


def shard_levels(stream_key, shape, cuts, least, top_value):
    factor_of = 1.0
    for dim, blocks in cuts:
        steps = jax.random.uniform(jax.random.fold_in(jax.random.fold_in(stream_key, 6), dim), (blocks,), jnp.float32, least / len(cuts), top_value / len(cuts))
        factor_of = factor_of * jnp.repeat(jnp.exp(steps), shape[dim] // blocks).reshape((-1,) + (1,) * (len(shape) - 1 - dim))
    return factor_of


def scatter_about(stream_key, dims, scale, limit, shards=(), kind=jnp.bfloat16):
    level = shard_levels(stream_key, dims, shards, -0.22, 0.18) if shards else 1.0
    values = jax.random.normal(stream_key, dims, jnp.float32) * scale * level
    return jnp.minimum(jnp.maximum(values, -limit), limit).astype(kind)


def setup_inputs(seed: int = 0, part: int = 0) -> dict:
    streams_of = jax.random.split(jax.random.key(seed), 11)
    part_splits = jax.random.split(jax.random.fold_in(streams_of[10], part), 11)
    features = scatter_about(part_splits[0], (FRAMES, C1, N_TILE, TILE_H, TILE_W), 1.0, 6.0, ((2, 16),))
    cache_first = scatter_about(part_splits[1], (2, C1, N_TILE, TILE_H, TILE_W), 1.0, 6.0, ((2, 16),))
    cache_second = scatter_about(part_splits[2], (2, C2, N_TILE, 2 * TILE_H, 2 * TILE_W), 1.0, 6.0, ((2, 16),))
    cache_third = scatter_about(part_splits[3], (2, C3, N_TILE, 4 * TILE_H, 4 * TILE_W), 1.0, 6.0, ((2, 16),))
    weight_first = scatter_about(streams_of[4], (3, 3, 3, C2, C1), (27 * C1) ** -0.5, 0.0625)
    weight_second = scatter_about(streams_of[5], (3, 3, 3, C3, C2), (27 * C2) ** -0.5, 0.078125)
    weight_third = scatter_about(streams_of[6], (3, 3, 3, RGB, C3), (27 * C3) ** -0.5, 0.125)
    gain_first = jnp.clip(1.0 + 0.18 * jax.random.normal(streams_of[7], (C1,), jnp.float32), 0.1, 1.9)
    gain_second = jnp.clip(1.0 + 0.18 * jax.random.normal(streams_of[8], (C2,), jnp.float32), 0.1, 1.9)
    gain_third = jnp.clip(1.0 + 0.18 * jax.random.normal(streams_of[9], (C3,), jnp.float32), 0.1, 1.9)
    return {"features": features, "cache_first": cache_first, "cache_second": cache_second, "cache_third": cache_third, "weight_first": weight_first, "weight_second": weight_second, "weight_third": weight_third, "gain_first": gain_first, "gain_second": gain_second, "gain_third": gain_third}


epsilon = 1e-06

def assemble(values):
    values = jnp.roll(values, TILES_X // 2, axis=2)
    frames, chans, count, height, width = values.shape
    tall = count // TILES_X
    grid = values.reshape(frames, chans, tall, TILES_X, height, width)
    return grid.transpose(0, 1, 2, 4, 3, 5).reshape(frames, chans, tall * height, TILES_X * width)

def split_tiles(values, height, width):
    frames, chans, total_rows, total_cols = values.shape
    grid = values.reshape(frames, chans, total_rows // height, height, TILES_X, width)
    tiled = grid.transpose(0, 1, 2, 4, 3, 5).reshape(frames, chans, total_rows // height * TILES_X, height, width)
    return jnp.roll(tiled, -(TILES_X // 2), axis=2)

def activate(values, gain):
    widened = values.astype(jnp.float32)
    meansq = lax.optimization_barrier(jnp.mean(widened * widened, axis=1, keepdims=True))
    normed = widened * lax.rsqrt(meansq + epsilon) * gain.astype(jnp.float32)[None, :, None, None]
    return jax.nn.silu(normed).astype(jnp.bfloat16)

def enlarge(values):
    return jnp.repeat(jnp.repeat(values, 2, axis=2), 2, axis=3)

def convolve(stacked, weight):
    frame_count = stacked.shape[0] - 2
    row_count = stacked.shape[2]
    col_count = stacked.shape[3]
    padded = jnp.pad(stacked, ((0, 0), (0, 0), (1, 1), (1, 1)))
    widened_weight = weight.astype(jnp.float32)

    def single(frame_index):
        slab = lax.dynamic_slice_in_dim(padded, frame_index, 3, 0).astype(jnp.float32)
        total = jnp.zeros((weight.shape[3], row_count, col_count), jnp.float32)
        for tap_time in range(3):
            for tap_row in range(3):
                for tap_col in range(3):
                    window = slab[tap_time, :, tap_row:tap_row + row_count, tap_col:tap_col + col_count]
                    total = total + jnp.einsum('oc,chw->ohw', widened_weight[tap_time, tap_row, tap_col], window)
        return total
    return lax.map(single, jnp.arange(frame_count, dtype=jnp.int32))

def reference(features, cache_first, cache_second, cache_third, weight_first, weight_second, weight_third, gain_first, gain_second, gain_third):
    inputs_first = activate(assemble(features), gain_first)
    out_first = convolve(jnp.concatenate([assemble(cache_first), inputs_first], 0), weight_first).astype(jnp.bfloat16)
    inputs_second = activate(enlarge(out_first), gain_second)
    out_second = convolve(jnp.concatenate([assemble(cache_second), inputs_second], 0), weight_second).astype(jnp.bfloat16)
    inputs_third = activate(enlarge(out_second), gain_third)
    result = convolve(jnp.concatenate([assemble(cache_third), inputs_third], 0), weight_third)
    return split_tiles(result, 4 * TILE_H, 4 * TILE_W)
```

```python
import functools

import jax
import jax.numpy as jnp
import numpy as np
from jax import lax
from jax.experimental import pallas as pl
from jax.experimental.pallas import tpu as pltpu
from jax.sharding import PartitionSpec as P

TILES_X = 8
EPS = 1e-06
F32 = jnp.float32
BF16 = jnp.bfloat16
PITCH = 24


def partner(index, size, odd):
    other = index ^ 1 if not odd else ((index - 1) ^ 1) + 1
    return other if 0 <= other < size and (not odd or index > 0) else index


def pairs_of(count, row_pair, col_pair):
    rows = count // TILES_X
    out = []
    for k in range(count):
        m = (k + TILES_X // 2) % count
        r, c = divmod(m, TILES_X)
        r2 = r if row_pair is None else partner(r, rows, row_pair)
        c2 = c if col_pair is None else partner(c, TILES_X, col_pair)
        if (row_pair is not None and r2 == r) or (col_pair is not None and c2 == c):
            r2, c2 = r, c
        out.append((k, (r2 * TILES_X + c2 - TILES_X // 2) % count))
    return out


def swap(values, count, row_pair, col_pair):
    return lax.ppermute(values, "tile", pairs_of(count, row_pair, col_pair))


def edge(values, axis, size, last):
    total = values.shape[axis]
    tail = lax.slice_in_dim(values, total - size, total, axis=axis)
    head = lax.slice_in_dim(values, 0, size, axis=axis)
    return jnp.where(last, tail, head)


def joined(second, third):
    gap = -second.shape[-1] % 128
    rest = -third.shape[-1] % 128
    return jnp.concatenate(
        [
            second,
            jnp.zeros(second.shape[:-1] + (gap,), second.dtype),
            third,
            jnp.zeros(third.shape[:-1] + (rest,), third.dtype),
        ],
        -1,
    )


@functools.lru_cache
def fine_taps(rgb):
    slots = np.zeros((2, 4, 3, 4, 4, 4, 2, 3, 3, 3, rgb), np.float32)
    for a in range(4):
        for d in range(3):
            row = (a + d - 1) // 2
            rs, half = {-1: (0, 1), 0: (0, 0), 1: (1, 1), 2: (1, 0)}[row]
            for b in range(4):
                for e in range(3):
                    cs = (b + e - 1) // 2 + 1
                    for t in range(3):
                        for c in range(rgb):
                            slots[rs, cs, 2 - t, b, c, a, half, t, d, e, c] += 1
    flat = slots.reshape(8 * 192, 2, 27 * rgb)
    return np.pad(flat, ((0, 0), (0, 0), (0, 96 - 27 * rgb))).reshape(8 * 192, 192)


@functools.lru_cache
def cache_taps(rgb):
    slots = np.zeros((6, 6, 2, 4, 4, 4, 3, 3, 3, rgb), np.float32)
    for a in range(4):
        for d in range(3):
            for b in range(4):
                for e in range(3):
                    for t in range(2):
                        for c in range(rgb):
                            slots[a + d, b + e, 1 - t, b, c, a, t, d, e, c] += 1
    flat = slots.reshape(36 * 128, 27 * rgb)
    return np.pad(flat, ((0, 0), (0, 96 - 27 * rgb)))


@functools.lru_cache
def spread(height, width):
    out = np.zeros((4, height, width, height, width, 4), np.float32)
    for b in range(4):
        for r in range(height):
            for c in range(width):
                out[b, r, c, r, c, b] = 1
    return out.reshape(4 * height * width, 4 * height * width)


def dot_nt(lhs, rhs):
    return lax.dot_general(lhs, rhs, (((1,), (1,)), ((), ())), preferred_element_type=F32)


def sides(flags):
    top, bottom, left, right, odd = (flags[i] for i in range(5))
    as_f = lambda v: v.astype(F32)
    return (
        as_f(top),
        as_f(bottom),
        (as_f(left * odd), as_f(left * (1 - odd))),
        (as_f(right * (1 - odd)), as_f(right * odd)),
    )


def history_kernel(
    flags, second, third, up2, down2, a2, b2, dau, dbu, dad, dbd, w2, w3, taps3, taps3c,
    part2, part3, wc2, wc3,
    e_lo, e_hi, e3, xc2, xc3, w3c,
):
    top, bottom, left, right = sides(flags)
    frames, tall, wide, chans = second.shape
    c3 = third.shape[-1]
    lo = 128
    hi = chans - lo
    read = lambda ref, *ix: ref[ix].astype(F32)

    w3c[...] = jnp.dot(taps3c[...], w3[0:96, 0:128], preferred_element_type=F32).astype(BF16)
    wc3[...] = jnp.dot(taps3[...], w3[96:288, :], preferred_element_type=F32).astype(BF16)
    for t in range(3):
        rows = {}
        for e in range(3):
            w = [w2[t, d, e].astype(F32) for d in range(3)]
            rows[e] = (w[0], w[0] + w[1], w[1] + w[2], w[2])
        for q in range(2):
            for cs in range(2):
                cols = [
                    rows[0][v] if (q, cs) == (0, 0) else rows[2][v] if (q, cs) == (1, 1)
                    else rows[1][v] + (rows[2][v] if q == 0 else rows[0][v])
                    for v in range(4)
                ]
                for rs in range(2):
                    base = ((t * 2 + q) * 2 + rs) * 2 + cs
                    wc2[base, 0:c3, :] = cols[2 * rs].astype(BF16)
                    wc2[base, c3:2 * c3, :] = cols[2 * rs + 1].astype(BF16)

    off = 8
    def put2(f, row, col, value):
        n = value.shape[0]
        e_lo[f, row, col:col + n, :] = value[:, :lo]
        e_hi[f, row, col:col + n, 0:hi] = value[:, lo:chans]
    for f in range(frames):
        for r in range(tall + 4):
            if r < 2:
                own = read(up2, f, r) * top
                pa, pb, s = read(dau, f, r), read(dbu, f, r), top
            elif r < tall + 2:
                own = read(second, f, r - 2)
                pa, pb, s = read(a2, f, r - 2), read(b2, f, r - 2), 1.0
            else:
                own = read(down2, f, r - tall - 2) * bottom
                pa, pb, s = read(dad, f, r - tall - 2), read(dbd, f, r - tall - 2), bottom
            put2(f, r, off, own)
            put2(f, r, off - 2, pa * (left[0] * s) + pb * (left[1] * s))
            put2(f, r, off + wide, pa * (right[0] * s) + pb * (right[1] * s))
    for k in range(4):
        for f in range(frames):
            for r in range(tall + 4):
                cols = pl.ds(off - 3 + k, PITCH, stride=2)
                xc2[k, f, r, :, 0:lo] = e_lo[f, r, cols, :].astype(BF16)
                xc2[k, f, r, :, lo:chans] = e_hi[f, r, cols, :].astype(BF16)[:, :hi]
    rows_out = tall + 2
    for q in range(2):
        acc = None
        for d in range(3):
            for e in range(3):
                lhs = xc2[e + q, :, d:d + rows_out].reshape(frames * rows_out * PITCH, chans)
                rhs = jnp.concatenate([w2[1, d, e], w2[0, d, e]], 0)
                term = dot_nt(lhs, rhs)
                acc = term if acc is None else acc + term
        acc = acc.reshape(frames, rows_out // 2, 2, PITCH, 2 * c3)
        v0 = acc[0, ..., c3:] + acc[1, ..., :c3]
        v1 = acc[1, ..., c3:]
        for o, v in enumerate((v0, v1)):
            part2[q, o] = jnp.concatenate([v[:, 1], v[:, 0]], -1)

    tall3, wide3 = third.shape[1:3]
    shift = 2 * 128
    def put3(f, row, col, value):
        n = value.shape[0]
        e3[f, row, col:col + n, 0:c3] = value
    for f in range(frames):
        for r in range(tall3):
            put3(f, r + 1, off, read(third, f, r))
        for j in range(2):
            half = wide3 // 2
            put3(f, 0, off + j * half, read(up2, f, j)[:, shift:shift + c3] * top)
            put3(f, tall3 + 1, off + j * half, read(down2, f, j)[:, shift:shift + c3] * bottom)
        for r in range(tall3 // 2):
            pa = read(a2, f, r)[:, shift:shift + c3]
            pb = read(b2, f, r)[:, shift:shift + c3]
            vl = pa * left[0] + pb * left[1]
            vr = pa * right[0] + pb * right[1]
            for j in range(2):
                put3(f, 1 + 2 * r + j, off - 1, vl[j:j + 1])
                put3(f, 1 + 2 * r + j, off + wide3, vr[j:j + 1])
        for row, da, db, s in ((0, dau, dbu, top), (tall3 + 1, dad, dbd, bottom)):
            pa = read(da, f, 0)[0:1, shift:shift + c3]
            pb = read(db, f, 0)[0:1, shift:shift + c3]
            put3(f, row, off - 1, pa * (left[0] * s) + pb * (left[1] * s))
            put3(f, row, off + wide3, pa * (right[0] * s) + pb * (right[1] * s))
    height, width = tall3 // 4, wide3 // 4
    lanes = lax.broadcasted_iota(jnp.int32, (width, 128), 1)
    for k in range(6):
        for f in range(frames):
            for r in range(tall3 + 2):
                value = e3[f, r, pl.ds(off - 1 + k, width, stride=4), :]
                xc3[k, f, r // 4, r % 4] = jnp.where(lanes < c3, value, 0.0).astype(BF16)
    acc = None
    for j in range(6):
        for k in range(0, 6, 2):
            lhs = jnp.concatenate(
                [
                    xc3[kk, :, j // 4:j // 4 + height, j % 4].reshape(frames * height * width, 128)
                    for kk in (k, k + 1)
                ],
                -1,
            )
            base = (j * 6 + k) * 128
            rhs = jnp.concatenate([w3c[base:base + 128], w3c[base + 128:base + 256]], -1)
            term = dot_nt(lhs, rhs)
            acc = term if acc is None else acc + term
    size = height * width
    part3[0] = acc[:size, 64:] + acc[size:, :64]
    part3[1] = acc[size:, 64:]


def normed(values, gain, total):
    meansq = jnp.sum(values * values, axis=-1, keepdims=True) * (1.0 / total)
    out = values * lax.rsqrt(meansq + EPS) * gain
    return out / (1.0 + jnp.exp(-out))


def frames_kernel(
    flags, feats, cache, up1, down1, a1, b1, dau, dbu, dad, dbd, w1, g1, g2, g3,
    part2, part3, wc2, wc3, spread_ref,
    out,
    e1, x1, e2, x2, x3,
):
    top, bottom, left, right = sides(flags)
    frames, height, width, chans = feats.shape
    old = cache.shape[0]
    total = frames + old
    c2 = wc2.shape[-1]
    c3 = c2 // 2
    read = lambda ref, *ix: ref[ix].astype(F32)

    off = 8
    for f in range(total):
        for r in range(height + 4):
            if r < 2:
                own = read(up1, f, r) * top
                pa, pb, s = read(dau, f, r), read(dbu, f, r), top
            elif r < height + 2:
                own = read(cache, f, r - 2) if f < old else read(feats, f - old, r - 2)
                pa, pb, s = read(a1, f, r - 2), read(b1, f, r - 2), 1.0
            else:
                own = read(down1, f, r - height - 2) * bottom
                pa, pb, s = read(dad, f, r - height - 2), read(dbd, f, r - height - 2), bottom
            e1[f, r, off:off + width, :] = own
            e1[f, r, off - 2:off, :] = pa * (left[0] * s) + pb * (left[1] * s)
            e1[f, r, off + width:off + width + 2, :] = pa * (right[0] * s) + pb * (right[1] * s)
    gain = g1[...]
    for f in range(old, total):
        for r in range(height + 4):
            e1[f, r] = normed(e1[f, r], gain, chans)
    for k in range(3):
        for f in range(total):
            for r in range(height + 4):
                x1[k, f, r] = e1[f, r, off - 2 + k:off - 2 + k + PITCH, :].astype(BF16)
    rows1 = height + 2
    acc = None
    for t in range(3):
        for d in range(3):
            for e in range(3):
                lhs = x1[e, t:t + frames, d:d + rows1].reshape(frames * rows1 * PITCH, chans)
                term = dot_nt(lhs, w1[t, d, e])
                acc = term if acc is None else acc + term
    acc = acc.reshape(frames, rows1, PITCH, c2)

    cols = lax.broadcasted_iota(jnp.int32, (PITCH, c2), 0)
    first = 1 - flags[2]
    last = width + flags[3]
    inside = (cols >= first) & (cols <= last)
    at_top = inside & (cols < flags[0] * PITCH)
    at_bottom = inside & (cols < flags[1] * PITCH)

    gain = g2[...]
    for f in range(frames):
        for r in range(rows1):
            keep = at_top if r == 0 else at_bottom if r == rows1 - 1 else inside
            value = jnp.where(keep, acc[f, r].astype(BF16).astype(F32), 0.0)
            e2[f, r, off:off + PITCH, :] = normed(value, gain, c2)
    for k in range(3):
        for f in range(frames):
            for r in range(rows1):
                x2[k, f, r] = e2[f, r, off - 1 + k:off - 1 + k + PITCH, :].astype(BF16)

    rows2 = height + 1
    lanes = lax.broadcasted_iota(jnp.int32, (PITCH, c2), 1)
    lower = lanes < c3
    gain = g3[...]
    for q in range(2):
        parts = []
        for t in range(3):
            count = frames - (2 - t)
            acc = None
            for rs in range(2):
                for cs in range(2):
                    lhs = x2[q + cs, 0:count, rs:rs + rows2].reshape(count * rows2 * PITCH, c2)
                    term = dot_nt(lhs, wc2[((t * 2 + q) * 2 + rs) * 2 + cs])
                    acc = term if acc is None else acc + term
            parts.append(acc.reshape(count, rows2, PITCH, c2))
        for f in range(frames):
            for r in range(rows2):
                value = parts[2][f, r]
                if f >= 1:
                    value = value + parts[1][f - 1, r]
                if f >= 2:
                    value = value + parts[0][f - 2, r]
                else:
                    value = value + part2[q, f, r]
                keep = inside
                if r == 0:
                    keep = (lower & inside) | at_top
                if r == rows2 - 1:
                    keep = (~lower & inside) | at_bottom
                value = jnp.where(keep, value.astype(BF16).astype(F32), 0.0)
                square = value * value
                sum_low = jnp.sum(jnp.where(lower, square, 0.0), axis=-1, keepdims=True)
                sum_high = jnp.sum(jnp.where(lower, 0.0, square), axis=-1, keepdims=True)
                scale = jnp.where(
                    lower,
                    lax.rsqrt(sum_low * (1.0 / c3) + EPS),
                    lax.rsqrt(sum_high * (1.0 / c3) + EPS),
                )
                value = value * scale * gain
                e2[f, r, off:off + PITCH, :] = value / (1.0 + jnp.exp(-value))
        for f in range(frames):
            for r in range(rows2):
                for cs in ((1, 3) if q == 0 else (0, 2)):
                    start = off + (0, 1, 1, 2)[cs]
                    x3[cs, f, r] = e2[f, r, start:start + width, :].astype(BF16)

    acc = None
    for rs in range(2):
        for cs in range(4):
            lhs = x3[cs, :, rs:rs + height].reshape(frames * height * width, c2)
            base = (rs * 4 + cs) * 192
            term = dot_nt(lhs, wc3[base:base + 192])
            acc = term if acc is None else acc + term
    size = height * width
    acc = acc.reshape(frames, size, 192)
    turned = []
    for f in range(frames):
        value = acc[f, :, 0:64]
        if f >= 1:
            value = value + acc[f - 1, :, 64:128]
        value = value + (acc[f - 2, :, 128:192] if f >= 2 else part3[f])
        value = value.T
        turned.append(jnp.concatenate([value[b * 16:(b + 1) * 16] for b in range(4)], -1))
    turned = jnp.concatenate(turned, 0)
    result = None
    for _ in range(3):
        piece = turned.astype(BF16)
        turned = turned - piece.astype(F32)
        term = jnp.dot(piece, spread_ref[...], preferred_element_type=F32)
        result = term if result is None else result + term
    for f in range(frames):
        for c in range(out.shape[1]):
            for r in range(height):
                out[f, c, 4 * r:4 * r + 4, :] = result[
                    f * 16 + c * 4:f * 16 + c * 4 + 4, r * 4 * width:(r + 1) * 4 * width
                ]


def body(count, features, cache_first, cache_second, cache_third, w1, w2, w3, g1, g2, g3):
    tile_rows = count // TILES_X
    place = (lax.axis_index("tile") + TILES_X // 2) % count
    col, row = place % TILES_X, place // TILES_X
    odd_col, odd_row = col % 2 == 1, row % 2 == 1
    flags = jnp.stack([row > 0, row < tile_rows - 1, col > 0, col < TILES_X - 1, odd_col]).astype(jnp.int32)

    last_dims = lambda v: v[:, :, 0].transpose(0, 2, 3, 1)
    feats, old1, old2, old3 = map(last_dims, (features, cache_first, cache_second, cache_third))
    frames, height, width, _ = feats.shape
    old = old1.shape[0]
    c2, c3 = old2.shape[-1], old3.shape[-1]

    def rows_of(values, size, odd):
        return edge(values, 1, size, odd_row if odd else ~odd_row)

    def cols_of(values, size, odd):
        return edge(values, 2, size, odd_col if odd else ~odd_col)

    def third_rows(values):
        return values.reshape(old, 2, -1, c3)

    def third_cols(values):
        return values.reshape(old, -1, 2, c3)

    def third_corner(values):
        return jnp.broadcast_to(values, (old, 2, 2, c3))

    row_pairs = [0] if tile_rows <= 2 else [0, 1]
    first = lambda f: jnp.concatenate([f(old1), f(feats)], 0)
    rows2, rows1, corners = {}, {}, {}
    for rp in row_pairs:
        rows2[rp] = swap(joined(rows_of(old2, 2, rp), third_rows(rows_of(old3, 1, rp))), count, rp, None)
    sent = {}
    for cp in (0, 1):
        x1 = first(lambda v: cols_of(v, 2, cp))
        x2 = joined(cols_of(old2, 2, cp), third_cols(cols_of(old3, 1, cp)))
        x1 = x1.reshape(-1, 2, x1.shape[-1])
        x2 = x2.reshape(-1, 2, x2.shape[-1])
        sent[cp] = swap(jnp.concatenate([x1, x2], 0), count, None, cp)
        for rp in row_pairs:
            y1 = first(lambda v: cols_of(rows_of(v, 2, rp), 2, cp))
            y2 = joined(
                cols_of(rows_of(old2, 2, rp), 2, cp),
                third_corner(cols_of(rows_of(old3, 1, rp), 1, cp)),
            )
            y1 = y1.reshape(-1, 2, y1.shape[-1])
            y2 = y2.reshape(-1, 2, y2.shape[-1])
            corners[rp, cp] = swap(jnp.concatenate([y1, y2], 0), count, rp, cp)
    for rp in row_pairs:
        rows1[rp] = swap(first(lambda v: rows_of(v, 2, rp)), count, rp, None)

    def above(pieces):
        return pieces[0] if len(pieces) == 1 else jnp.where(odd_row, pieces[0], pieces[1])

    def below(pieces):
        return pieces[0] if len(pieces) == 1 else jnp.where(odd_row, pieces[1], pieces[0])

    up1, down1 = above(rows1), below(rows1)
    up2, down2 = above(rows2), below(rows2)
    cut_side = (frames + old) * height
    cut_corner = (frames + old) * 2
    side1 = [sent[cp][:cut_side].reshape(frames + old, height, 2, -1) for cp in (0, 1)]
    side2 = [sent[cp][cut_side:].reshape(old, 2 * height, 2, -1) for cp in (0, 1)]
    diagonals = [
        pick({rp: corners[rp, cp] for rp in row_pairs}) for pick in (above, below) for cp in (0, 1)
    ]
    corner1 = [v[:cut_corner].reshape(frames + old, 2, 2, -1) for v in diagonals]
    corner2 = [v[cut_corner:].reshape(old, 2, 2, -1) for v in diagonals]

    rgb = w3.shape[3]
    flat3 = w3.reshape(27 * rgb, c3)
    flat3 = jnp.pad(flat3, ((0, 96 - 27 * rgb), (0, 0)))
    w3_all = jnp.concatenate(
        [
            jnp.pad(flat3, ((0, 0), (0, 192 - c3))),
            jnp.pad(flat3, ((0, 0), (0, 192 - c3))),
            jnp.pad(flat3, ((0, 0), (c3, 192 - 2 * c3))),
        ],
        0,
    )

    smem = pl.BlockSpec(memory_space=pltpu.SMEM)
    vmem = pl.BlockSpec(memory_space=pltpu.VMEM)
    size = height * width
    part2, part3, wc2, wc3 = pl.pallas_call(
        history_kernel,
        out_shape=[
            jax.ShapeDtypeStruct((2, 2, height + 1, PITCH, c2), F32),
            jax.ShapeDtypeStruct((2, size, 64), F32),
            jax.ShapeDtypeStruct((24, 2 * c3, c2), BF16),
            jax.ShapeDtypeStruct((8 * 192, 192), BF16),
        ],
        in_specs=[smem] + [vmem] * 14,
        out_specs=[vmem] * 4,
        scratch_shapes=[
            pltpu.VMEM((old, 2 * height + 4, 64, 128), F32),
            pltpu.VMEM((old, 2 * height + 4, 64, 128), F32),
            pltpu.VMEM((old, 4 * height + 2, 96, 128), F32),
            pltpu.VMEM((4, old, 2 * height + 4, PITCH, c2), BF16),
            pltpu.VMEM((6, old, height + 1, 4, width, 128), BF16),
            pltpu.VMEM((36 * 128, 128), BF16),
        ],
        compiler_params=pltpu.CompilerParams(vmem_limit_bytes=60 << 20),
        cost_estimate=pl.CostEstimate(flops=4_000_000_000, bytes_accessed=4_000_000, transcendentals=0),
        name="history",
    )(
        flags, old2, old3, up2, down2, *side2, *corner2, w2, w3_all,
        jnp.asarray(fine_taps(rgb), BF16), jnp.asarray(cache_taps(rgb), BF16),
    )

    out = pl.pallas_call(
        frames_kernel,
        out_shape=jax.ShapeDtypeStruct((frames, rgb, 4 * height, 4 * width), F32),
        in_specs=[smem] + [vmem] * 19,
        out_specs=vmem,
        scratch_shapes=[
            pltpu.VMEM((frames + old, height + 4, 40, feats.shape[-1]), F32),
            pltpu.VMEM((3, frames + old, height + 4, PITCH, feats.shape[-1]), BF16),
            pltpu.VMEM((frames, height + 2, 40, c2), F32),
            pltpu.VMEM((3, frames, height + 2, PITCH, c2), BF16),
            pltpu.VMEM((4, frames, height + 1, width, c2), BF16),
        ],
        compiler_params=pltpu.CompilerParams(vmem_limit_bytes=60 << 20),
        cost_estimate=pl.CostEstimate(flops=10_000_000_000, bytes_accessed=8_000_000, transcendentals=0),
        name="frames",
    )(
        flags, feats, old1, up1, down1, *side1, *corner1, w1, g1[None], g2[None],
        jnp.concatenate([g3, g3])[None], part2, part3, wc2, wc3,
        jnp.asarray(spread(height, width), BF16),
    )
    return out[:, :, None]


def solution(mesh):
    tiled = P("groups", None, "tile", None, None)
    return jax.shard_map(
        functools.partial(body, mesh.shape["tile"]),
        mesh=mesh,
        in_specs=(tiled,) * 4 + (P(),) * 6,
        out_specs=tiled,
        check_vma=False,
    )
```

```python
import functools

import jax
import jax.numpy as jnp
import numpy as np
from jax import lax
from jax.experimental import pallas as pl
from jax.experimental.pallas import tpu as pltpu
from jax.sharding import PartitionSpec as P


TILES_X = 8
EPS = 1e-06
F32 = jnp.float32
BF16 = jnp.bfloat16
PITCH = 24


def partner(index, size, odd):
    other = index ^ 1 if not odd else ((index - 1) ^ 1) + 1
    return other if 0 <= other < size and (not odd or index > 0) else index


def pairs_of(count, row_pair, col_pair):
    rows = count // TILES_X
    out = []
    for k in range(count):
        m = (k + TILES_X // 2) % count
        r, c = divmod(m, TILES_X)
        r2 = r if row_pair is None else partner(r, rows, row_pair)
        c2 = c if col_pair is None else partner(c, TILES_X, col_pair)
        if (row_pair is not None and r2 == r) or (col_pair is not None and c2 == c):
            r2, c2 = r, c
        out.append((k, (r2 * TILES_X + c2 - TILES_X // 2) % count))
    return out


def swap(values, count, row_pair, col_pair):
    return lax.ppermute(values, "tile", pairs_of(count, row_pair, col_pair))


@functools.lru_cache
def fine_taps(rgb):
    slots = np.zeros((2, 4, 3, 4, 4, 4, 2, 3, 3, 3, rgb), np.float32)
    for a in range(4):
        for d in range(3):
            row = (a + d - 1) // 2
            rs, half = {-1: (0, 1), 0: (0, 0), 1: (1, 1), 2: (1, 0)}[row]
            for b in range(4):
                for e in range(3):
                    cs = (b + e - 1) // 2 + 1
                    for t in range(3):
                        for c in range(rgb):
                            slots[rs, cs, 2 - t, b, c, a, half, t, d, e, c] += 1
    flat = slots.reshape(8 * 192, 2, 27 * rgb)
    return np.pad(flat, ((0, 0), (0, 0), (0, 96 - 27 * rgb))).reshape(8 * 192, 192)


@functools.lru_cache
def cache_taps(rgb):
    slots = np.zeros((6, 6, 2, 4, 4, 4, 3, 3, 3, rgb), np.float32)
    for a in range(4):
        for d in range(3):
            for b in range(4):
                for e in range(3):
                    for t in range(2):
                        for c in range(rgb):
                            slots[a + d, b + e, 1 - t, b, c, a, t, d, e, c] += 1
    flat = slots.reshape(36 * 128, 27 * rgb)
    return np.pad(flat, ((0, 0), (0, 96 - 27 * rgb)))


@functools.lru_cache
def spread(height, width):
    out = np.zeros((4, height, width, height, width, 4), np.float32)
    for b in range(4):
        for r in range(height):
            for c in range(width):
                out[b, r, c, r, c, b] = 1
    return out.reshape(4 * height * width, 4 * height * width)


def dot_nt(lhs, rhs):
    return lax.dot_general(lhs, rhs, (((1,), (1,)), ((), ())), preferred_element_type=F32)


def position(count):
    place = lax.rem(lax.axis_index("tile") + TILES_X // 2, count)
    col, row = lax.rem(place, TILES_X), lax.div(place, TILES_X)
    flag = lambda v: v.astype(jnp.int32)
    return (
        flag(row > 0), flag(row < count // TILES_X - 1), flag(col > 0), flag(col < TILES_X - 1),
        lax.rem(col, 2), lax.rem(row, 2),
    )


def sides(flags):
    top, bottom, left, right, odd = flags[:5]
    as_f = lambda v: v.astype(F32)
    return (
        as_f(top),
        as_f(bottom),
        (as_f(left * odd), as_f(left * (1 - odd))),
        (as_f(right * (1 - odd)), as_f(right * odd)),
    )


def pack_kernel(count, row_pairs, feats_hbm, old1_hbm, old2_hbm, old3_hbm, *refs):
    *outs, feats, old1, old2, old3, near3, far3, sems = refs
    wide3 = old3_hbm.shape[2]
    copies = [
        pltpu.make_async_copy(src, dst, sems.at[i])
        for i, (src, dst) in enumerate((
            (feats_hbm, feats), (old1_hbm, old1), (old2_hbm, old2),
            (old3_hbm.at[:, pl.ds(0, 1)], old3.at[:, pl.ds(0, 1)]),
            (old3_hbm.at[:, pl.ds(old3_hbm.shape[1] - 1, 1)], old3.at[:, pl.ds(1, 1)]),
            (old3_hbm.at[:, :, pl.ds(0, 8)], near3),
            (old3_hbm.at[:, :, pl.ds(wide3 - 8, 8)], far3),
        ))
    ]
    for copy in copies:
        copy.start()
    *_, odd_col, odd_row = position(count)
    for copy in copies:
        copy.wait()
    firsts = [old1.at[f] for f in range(old1.shape[0])] + [feats.at[f] for f in range(feats.shape[0])]
    _, height, width, _ = feats.shape
    c2, c3 = old2.shape[-1], old3.shape[-1]
    aside = slice(256, 256 + c3)
    total = len(firsts)
    outs = list(outs)
    sides_out = {0: outs.pop(0), 1: outs.pop(0)}
    for rp in row_pairs:
        rows2, rows1 = outs.pop(0), outs.pop(0)
        low = odd_row if rp else 1 - odd_row
        start1, start2, start3 = low * (height - 2), low * (2 * height - 2), low
        for i, ref in enumerate(firsts):
            rows1[i] = ref[pl.ds(start1, 2)]
        half = 2 * width
        for f in range(old2.shape[0]):
            rows2[f, :, :, 0:c2] = old2[f, pl.ds(start2, 2)]
            for j in range(2):
                rows2[f, j, :, aside] = old3[f, start3, j * half:(j + 1) * half, :]
        for cp in (0, 1):
            corner = outs.pop(0)
            far = odd_col if cp else 1 - odd_col
            for value in (0, 1):
                @pl.when(far == value)
                def _():
                    pick = lambda n, size: slice(value * (n - size), value * (n - size) + size)
                    for i, ref in enumerate(firsts):
                        corner[2 * i:2 * i + 2] = ref[pl.ds(start1, 2), pick(width, 2), :]
                    for f in range(old2.shape[0]):
                        at = 2 * total + 2 * f
                        corner[at:at + 2, :, 0:c2] = old2[f, pl.ds(start2, 2), pick(2 * width, 2), :]
                        corner[at, 0:1, aside] = old3[f, start3, pick(wide3, 1), :]
    for cp in (0, 1):
        side = sides_out[cp]
        far = odd_col if cp else 1 - odd_col
        for value in (0, 1):
            @pl.when(far == value)
            def _():
                pick = lambda n, size: slice(value * (n - size), value * (n - size) + size)
                for i, ref in enumerate(firsts):
                    side[height * i:height * (i + 1)] = ref[:, pick(width, 2), :]
                for f in range(old2.shape[0]):
                    at = height * total + 2 * height * f
                    side[at:at + 2 * height, :, 0:c2] = old2[f, :, pick(2 * width, 2), :]
                    for r in range(2 * height):
                        ends = near3 if value == 0 else far3
                        pair = [ends[f, 2 * r + j, pick(8, 1), :].astype(F32) for j in range(2)]
                        side[at + r, :, aside] = jnp.concatenate(pair, 0).astype(BF16)


def weights_kernel(w2, w3, taps3, taps3c, wc2, wc3, w3c, flat):
    c3 = w2.shape[3]
    rgb = w3.shape[3]
    flat[...] = jnp.zeros_like(flat)
    for t in range(3):
        for d in range(3):
            for e in range(3):
                row = ((t * 3 + d) * 3 + e) * rgb
                value = w3[t, d, e].astype(F32)
                flat[row:row + rgb, 0:c3] = value
                flat[96 + row:96 + row + rgb, c3:2 * c3] = value
    three = flat[0:96, 0:128].astype(BF16)
    w3c[...] = jnp.dot(taps3c[...], three, preferred_element_type=F32).astype(BF16)
    wc3[:, 0:2 * c3] = jnp.dot(taps3[...], flat[...].astype(BF16), preferred_element_type=F32).astype(BF16)
    for t in range(3):
        rows = {}
        for e in range(3):
            w = [w2[t, d, e].astype(F32) for d in range(3)]
            rows[e] = (w[0], w[0] + w[1], w[1] + w[2], w[2])
        for q in range(2):
            for cs in range(2):
                cols = [
                    rows[0][v] if (q, cs) == (0, 0) else rows[2][v] if (q, cs) == (1, 1)
                    else rows[1][v] + (rows[2][v] if q == 0 else rows[0][v])
                    for v in range(4)
                ]
                for rs in range(2):
                    base = ((t * 2 + q) * 2 + rs) * 2 + cs
                    wc2[base, 0:c3, 0:2 * c3] = cols[2 * rs].astype(BF16)
                    wc2[base, c3:2 * c3, 0:2 * c3] = cols[2 * rs + 1].astype(BF16)
    lanes = wc2.shape[-1]
    wc2[:, :, 2 * c3:lanes] = jnp.zeros(wc2.shape[:2] + (lanes - 2 * c3,), BF16)
    wc3[:, 2 * c3:lanes] = jnp.zeros((wc3.shape[0], lanes - 2 * c3), BF16)


def history_kernel(
    count, second, third, up2, down2, side_a, side_b, dau, dbu, dad, dbd, w2, w3c,
    part2, part3,
    e_lo, e_hi, e3, xc2, xc3,
):
    top, bottom, left, right = sides(position(count))
    frames, tall, wide, chans = second.shape
    c3 = third.shape[-1]
    lo = 128
    hi = chans - lo
    read = lambda ref, *ix: ref[ix].astype(F32)
    skip = side_a.shape[0] - frames * tall
    skip_corner = dau.shape[0] - frames * 2
    at_side = lambda ref, f, r: read(ref, skip + f * tall + r)
    at_corner = lambda ref, f, r: read(ref, skip_corner + 2 * f + r)

    off = 8

    def put2(f, row, col, value):
        n = value.shape[0]
        e_lo[f, row, col:col + n, :] = value[:, :lo]
        e_hi[f, row, col:col + n, 0:hi] = value[:, lo:chans]

    for f in range(frames):
        for r in range(tall + 4):
            if r < 2:
                own = read(up2, f, r) * top
                pa, pb, s = at_corner(dau, f, r), at_corner(dbu, f, r), top
            elif r < tall + 2:
                own = read(second, f, r - 2)
                pa, pb, s = at_side(side_a, f, r - 2), at_side(side_b, f, r - 2), 1.0
            else:
                own = read(down2, f, r - tall - 2) * bottom
                pa, pb, s = at_corner(dad, f, r - tall - 2), at_corner(dbd, f, r - tall - 2), bottom
            put2(f, r, off, own)
            put2(f, r, off - 2, pa * (left[0] * s) + pb * (left[1] * s))
            put2(f, r, off + wide, pa * (right[0] * s) + pb * (right[1] * s))
    for k in range(4):
        for f in range(frames):
            for r in range(tall + 4):
                cols = pl.ds(off - 3 + k, PITCH, stride=2)
                xc2[k, f, r, :, 0:lo] = e_lo[f, r, cols, :].astype(BF16)
                xc2[k, f, r, :, lo:chans] = e_hi[f, r, cols, :].astype(BF16)[:, :hi]
    rows_out = tall + 2
    for q in range(2):
        acc = None
        for d in range(3):
            for e in range(3):
                lhs = xc2[e + q, :, d:d + rows_out].reshape(frames * rows_out * PITCH, chans)
                rhs = jnp.concatenate([w2[1, d, e], w2[0, d, e]], 0)
                term = dot_nt(lhs, rhs)
                acc = term if acc is None else acc + term
        acc = acc.reshape(frames, rows_out // 2, 2, PITCH, 2 * c3)
        v0 = acc[0, ..., c3:] + acc[1, ..., :c3]
        v1 = acc[1, ..., c3:]
        for o, v in enumerate((v0, v1)):
            part2[q, o] = jnp.concatenate([v[:, 1], v[:, 0]], -1)

    tall3, wide3 = third.shape[1:3]
    shift = 2 * 128

    def put3(f, row, col, value):
        n = value.shape[0]
        e3[f, row, col:col + n, 0:c3] = value

    for f in range(frames):
        for r in range(tall3):
            put3(f, r + 1, off, read(third, f, r))
        for j in range(2):
            half = wide3 // 2
            put3(f, 0, off + j * half, read(up2, f, j)[:, shift:shift + c3] * top)
            put3(f, tall3 + 1, off + j * half, read(down2, f, j)[:, shift:shift + c3] * bottom)
        for r in range(tall3 // 2):
            pa = at_side(side_a, f, r)[:, shift:shift + c3]
            pb = at_side(side_b, f, r)[:, shift:shift + c3]
            vl = pa * left[0] + pb * left[1]
            vr = pa * right[0] + pb * right[1]
            for j in range(2):
                put3(f, 1 + 2 * r + j, off - 1, vl[j:j + 1])
                put3(f, 1 + 2 * r + j, off + wide3, vr[j:j + 1])
        for row, da, db, s in ((0, dau, dbu, top), (tall3 + 1, dad, dbd, bottom)):
            pa = at_corner(da, f, 0)[0:1, shift:shift + c3]
            pb = at_corner(db, f, 0)[0:1, shift:shift + c3]
            put3(f, row, off - 1, pa * (left[0] * s) + pb * (left[1] * s))
            put3(f, row, off + wide3, pa * (right[0] * s) + pb * (right[1] * s))
    height, width = tall3 // 4, wide3 // 4
    lanes = lax.broadcasted_iota(jnp.int32, (width, 128), 1)
    for k in range(6):
        for f in range(frames):
            for r in range(tall3 + 2):
                value = e3[f, r, pl.ds(off - 1 + k, width, stride=4), :]
                xc3[k, f, r // 4, r % 4] = jnp.where(lanes < c3, value, 0.0).astype(BF16)
    acc = None
    for j in range(6):
        for k in range(0, 6, 2):
            lhs = jnp.concatenate(
                [
                    xc3[kk, :, j // 4:j // 4 + height, j % 4].reshape(frames * height * width, 128)
                    for kk in (k, k + 1)
                ],
                -1,
            )
            base = (j * 6 + k) * 128
            rhs = jnp.concatenate([w3c[base:base + 128], w3c[base + 128:base + 256]], -1)
            term = dot_nt(lhs, rhs)
            acc = term if acc is None else acc + term
    size = height * width
    part3[0] = acc[:size, 64:] + acc[size:, :64]
    part3[1] = acc[size:, 64:]


def normed(values, gain, total):
    meansq = jnp.sum(values * values, axis=-1, keepdims=True) * (1.0 / total)
    out = values * lax.rsqrt(meansq + EPS) * gain
    return out / (1.0 + jnp.exp(-out))


def frames_kernel(
    count, feats, cache, up1, down1, side_a, side_b, dau, dbu, dad, dbd, w1, g1, g2, g3,
    part2, part3, wc2, wc3, spread_ref,
    out,
    e1, x1, e2, x2, x3,
):
    flags = position(count)
    top, bottom, left, right = sides(flags)
    frames, height, width, chans = feats.shape
    old = cache.shape[0]
    total = frames + old
    c2 = g2.shape[0]
    c3 = c2 // 2
    read = lambda ref, *ix: ref[ix].astype(F32)

    off = 8
    rows1, rows2 = height + 2, height + 1
    lanes2 = e2.shape[-1]
    always = flags[2] + flags[3] > 0

    cols = lax.broadcasted_iota(jnp.int32, (PITCH, c2), 0)
    first = 1 - flags[2]
    last = width + flags[3]
    inside = (cols >= first) & (cols <= last)
    at_top = inside & (cols < flags[0] * PITCH)
    at_bottom = inside & (cols < flags[1] * PITCH)

    @pl.when(always)
    def _():
        for f in range(total):
            for r in range(height + 4):
                if r < 2:
                    own = read(up1, f, r) * top
                    pa, pb, s = read(dau, 2 * f + r), read(dbu, 2 * f + r), top
                elif r < height + 2:
                    own = read(cache, f, r - 2) if f < old else read(feats, f - old, r - 2)
                    pa, pb, s = read(side_a, f * height + r - 2), read(side_b, f * height + r - 2), 1.0
                else:
                    own = read(down1, f, r - height - 2) * bottom
                    at = 2 * f + r - height - 2
                    pa, pb, s = read(dad, at), read(dbd, at), bottom
                e1[f, r, off:off + width, :] = own
                e1[f, r, off - 2:off, :] = pa * (left[0] * s) + pb * (left[1] * s)
                e1[f, r, off + width:off + width + 2, :] = pa * (right[0] * s) + pb * (right[1] * s)
        gain = g1[...].reshape(1, chans)
        for f in range(old, total):
            for r in range(height + 4):
                e1[f, r] = normed(e1[f, r], gain, chans)
        for k in range(3):
            for f in range(total):
                for r in range(height + 4):
                    x1[k, f, r] = e1[f, r, off - 2 + k:off - 2 + k + PITCH, :].astype(BF16)

    @pl.when(always)
    def _():
        pieces = [
            (t, d, e, slice(i, i + 128))
            for t in range(3) for d in range(3) for e in range(3) for i in range(0, chans, 128)
        ]
        half = frames // 2
        accs = [None, None]
        for i in range(0, len(pieces), 4):
            rhs = jnp.concatenate([w1[t, d, e, :, ch] for t, d, e, ch in pieces[i:i + 4]], -1)
            for h in range(2):
                lhs = [
                    x1[e, t + h * half:t + h * half + half, d:d + rows1, :, ch].reshape(-1, 128)
                    for t, d, e, ch in pieces[i:i + 4]
                ]
                term = dot_nt(jnp.concatenate(lhs, -1), rhs)
                accs[h] = term if accs[h] is None else accs[h] + term
        accs = [v.reshape(half, rows1, PITCH, c2) for v in accs]

        gain = g2[...].reshape(1, c2)
        e2[:, :, :, c2:lanes2] = jnp.zeros(e2.shape[:3] + (lanes2 - c2,), F32)
        for f in range(frames):
            for r in range(rows1):
                keep = at_top if r == 0 else at_bottom if r == rows1 - 1 else inside
                value = jnp.where(keep, accs[f // half][f % half, r].astype(BF16).astype(F32), 0.0)
                e2[f, r, off:off + PITCH, 0:c2] = normed(value, gain, c2)
        for k in range(3):
            for f in range(frames):
                for r in range(rows1):
                    x2[k, f, r] = e2[f, r, off - 1 + k:off - 1 + k + PITCH, :].astype(BF16)

    @pl.when(always)
    def _():
        lanes = lax.broadcasted_iota(jnp.int32, (PITCH, c2), 1)
        lower = lanes < c3
        gain = jnp.concatenate([g3[...].reshape(1, c3)] * 2, -1)
        every = ([], [])
        for t in range(3):
            count = frames - (2 - t)
            accs = [None, None]
            for rs in range(2):
                for q in range(2):
                    lhs = [
                        x2[q + cs, 0:count, rs:rs + rows2].reshape(count * rows2 * PITCH, lanes2)
                        for cs in range(2)
                    ]
                    base = ((t * 2 + q) * 2 + rs) * 2
                    term = dot_nt(jnp.concatenate(lhs, -1), jnp.concatenate([wc2[base], wc2[base + 1]], -1))
                    accs[q] = term if accs[q] is None else accs[q] + term
            for q in range(2):
                every[q].append(accs[q].reshape(count, rows2, PITCH, c2))
        for q in range(2):
            parts = every[q]
            for f in range(frames):
                for r in range(rows2):
                    value = parts[2][f, r]
                    if f >= 1:
                        value = value + parts[1][f - 1, r]
                    if f >= 2:
                        value = value + parts[0][f - 2, r]
                    else:
                        value = value + part2[q, f, r]
                    keep = inside
                    if r == 0:
                        keep = (lower & inside) | at_top
                    if r == rows2 - 1:
                        keep = (~lower & inside) | at_bottom
                    value = jnp.where(keep, value.astype(BF16).astype(F32), 0.0)
                    square = value * value
                    sum_low = jnp.sum(jnp.where(lower, square, 0.0), axis=-1, keepdims=True)
                    sum_high = jnp.sum(jnp.where(lower, 0.0, square), axis=-1, keepdims=True)
                    scale = jnp.where(
                        lower,
                        lax.rsqrt(sum_low * (1.0 / c3) + EPS),
                        lax.rsqrt(sum_high * (1.0 / c3) + EPS),
                    )
                    value = value * scale * gain
                    e2[f, r, off:off + PITCH, 0:c2] = value / (1.0 + jnp.exp(-value))
            for f in range(frames):
                for r in range(rows2):
                    for cs in ((1, 3) if q == 0 else (0, 2)):
                        start = off + (0, 1, 1, 2)[cs]
                        x3[cs, f, r] = e2[f, r, start:start + width, :].astype(BF16)

    @pl.when(always)
    def _():
        acc = None
        for rs in range(2):
            for cs in (0, 2):
                lhs = [
                    x3[i, :, rs:rs + height].reshape(frames * height * width, lanes2) for i in (cs, cs + 1)
                ]
                base = (rs * 4 + cs) * 192
                rhs = [wc3[base:base + 192], wc3[base + 192:base + 384]]
                term = dot_nt(jnp.concatenate(lhs, -1), jnp.concatenate(rhs, -1))
                acc = term if acc is None else acc + term
        size = height * width
        acc = acc.reshape(frames, size, 192)
        turned = []
        for f in range(frames):
            value = acc[f, :, 0:64]
            if f >= 1:
                value = value + acc[f - 1, :, 64:128]
            value = value + (acc[f - 2, :, 128:192] if f >= 2 else part3[f])
            value = value.T
            turned.append(jnp.concatenate([value[b * 16:(b + 1) * 16] for b in range(4)], -1))
        turned = jnp.concatenate(turned, 0)
        result = None
        for _ in range(3):
            piece = turned.astype(BF16)
            turned = turned - piece.astype(F32)
            term = jnp.dot(piece, spread_ref[...], preferred_element_type=F32)
            result = term if result is None else result + term
        for f in range(frames):
            for c in range(out.shape[1]):
                for r in range(height):
                    out[f, c, 4 * r:4 * r + 4, :] = result[
                        f * 16 + c * 4:f * 16 + c * 4 + 4, r * 4 * width:(r + 1) * 4 * width
                    ]


def body(count, features, cache_first, cache_second, cache_third, w1, w2, w3, g1, g2, g3):
    tile_rows = count // TILES_X
    last_dims = lambda v: v[:, :, 0].transpose(0, 2, 3, 1)
    feats, old1, old2, old3 = map(last_dims, (features, cache_first, cache_second, cache_third))
    frames, height, width, c1 = feats.shape
    old = old1.shape[0]
    total = frames + old
    c2, c3 = old2.shape[-1], old3.shape[-1]
    rgb = w3.shape[3]
    row_pairs = [0] if tile_rows <= 2 else [0, 1]
    vmem = pl.BlockSpec(memory_space=pltpu.VMEM)
    bf = lambda *shape: jax.ShapeDtypeStruct(shape, BF16)

    def call(kernel, ins, outs, scratch, limit, flops, space=vmem):
        return pl.pallas_call(
            kernel,
            out_shape=outs,
            in_specs=[space] * len(ins),
            out_specs=[vmem] * len(outs),
            scratch_shapes=scratch,
            compiler_params=pltpu.CompilerParams(vmem_limit_bytes=int(limit * 2**20)),
            cost_estimate=pl.CostEstimate(flops=flops, bytes_accessed=2_000_000, transcendentals=0),
        )(*ins)

    side = bf(total * height + old * 2 * height, 2, c1)
    corner = bf(total * 2 + old * 2, 2, c1)
    rows = [bf(old, 2, 2 * width, c1), bf(total, 2, width, c1)]
    packed = call(
        functools.partial(pack_kernel, count, row_pairs), (feats, old1, old2, old3),
        [side] * 2 + (rows + [corner] * 2) * len(row_pairs),
        [
            pltpu.VMEM(feats.shape, BF16),
            pltpu.VMEM(old1.shape, BF16),
            pltpu.VMEM(old2.shape, BF16),
            pltpu.VMEM((old, 2, 4 * width, c3), BF16),
            pltpu.VMEM((old, 4 * height, 8, c3), BF16),
            pltpu.VMEM((old, 4 * height, 8, c3), BF16),
            pltpu.SemaphoreType.DMA((7,)),
        ],
        62.9, 100_000_000, pl.BlockSpec(memory_space=pltpu.HBM),
    )

    sent = [swap(packed[cp], count, None, cp) for cp in (0, 1)]
    rows1, rows2, corners = [], [], ([], [])
    for i, rp in enumerate(row_pairs):
        piece = packed[2 + 4 * i:6 + 4 * i]
        rows2.append(swap(piece[0], count, rp, None))
        for cp in (0, 1):
            corners[cp].append(swap(piece[2 + cp], count, rp, cp))
        rows1.append(swap(piece[1], count, rp, None))
    odd_row = (lax.axis_index("tile") + TILES_X // 2) // TILES_X % 2 == 1

    def above(pieces):
        return pieces[0] if len(pieces) == 1 else jnp.where(odd_row, pieces[0], pieces[1])

    def below(pieces):
        return pieces[0] if len(pieces) == 1 else jnp.where(odd_row, pieces[1], pieces[0])

    diagonals = [pick(corners[cp]) for pick in (above, below) for cp in (0, 1)]
    size = height * width
    wc2, wc3, w3c = call(
        weights_kernel,
        (w2, w3, jnp.asarray(fine_taps(rgb), BF16), jnp.asarray(cache_taps(rgb), BF16)),
        [bf(24, 2 * c3, 256), bf(8 * 192, 256), bf(36 * 128, 128)],
        [pltpu.VMEM((192, 192), F32)], 16, 500_000_000,
    )
    part2, part3 = call(
        functools.partial(history_kernel, count),
        (old2, old3, above(rows2), below(rows2), *sent, *diagonals, w2, w3c),
        [
            jax.ShapeDtypeStruct((2, 2, height + 1, PITCH, c2), F32),
            jax.ShapeDtypeStruct((2, size, 64), F32),
        ],
        [
            pltpu.VMEM((old, 2 * height + 4, 64, 128), F32),
            pltpu.VMEM((old, 2 * height + 4, 64, 128), F32),
            pltpu.VMEM((old, 4 * height + 2, 96, 128), F32),
            pltpu.VMEM((4, old, 2 * height + 4, PITCH, c2), BF16),
            pltpu.VMEM((6, old, height + 1, 4, width, 128), BF16),
        ],
        22, 4_000_000_000,
    )
    (out,) = call(
        functools.partial(frames_kernel, count),
        (
            feats, old1, above(rows1), below(rows1), *sent, *diagonals, w1, g1, g2, g3,
            part2, part3, wc2, wc3, jnp.asarray(spread(height, width), BF16),
        ),
        [jax.ShapeDtypeStruct((frames, rgb, 4 * height, 4 * width), F32)],
        [
            pltpu.VMEM((total, height + 4, 40, c1), F32),
            pltpu.VMEM((3, total, height + 4, PITCH, c1), BF16),
            pltpu.VMEM((frames, height + 2, 40, 256), F32),
            pltpu.VMEM((3, frames, height + 2, PITCH, 256), BF16),
            pltpu.VMEM((4, frames, height + 1, width, 256), BF16),
        ],
        26, 10_000_000_000,
    )
    return out[:, :, None]


def solution(mesh):
    tiled = P("groups", None, "tile", None, None)
    return jax.shard_map(
        functools.partial(body, mesh.shape["tile"]),
        mesh=mesh,
        in_specs=(tiled,) * 4 + (P(),) * 6,
        out_specs=tiled,
        check_vma=False,
    )
```

```python
import functools

import jax
import jax.numpy as jnp
from jax import lax
from jax.experimental import pallas as pl
from jax.experimental.pallas import tpu as pltpu
from jax.sharding import PartitionSpec as P


TILES_X = 8
EPS = 1e-06
F32 = jnp.float32
BF16 = jnp.bfloat16
PITCH = 24


def partner(index, size, odd):
    other = index ^ 1 if not odd else ((index - 1) ^ 1) + 1
    return other if 0 <= other < size and (not odd or index > 0) else index


def pairs_of(count, row_pair, col_pair):
    rows = count // TILES_X
    out = []
    for k in range(count):
        m = (k + TILES_X // 2) % count
        r, c = divmod(m, TILES_X)
        r2 = r if row_pair is None else partner(r, rows, row_pair)
        c2 = c if col_pair is None else partner(c, TILES_X, col_pair)
        if (row_pair is not None and r2 == r) or (col_pair is not None and c2 == c):
            r2, c2 = r, c
        out.append((k, (r2 * TILES_X + c2 - TILES_X // 2) % count))
    return out


def swap(values, count, row_pair, col_pair):
    return lax.ppermute(values, "tile", pairs_of(count, row_pair, col_pair))


def dot_nt(lhs, rhs):
    return lax.dot_general(lhs, rhs, (((1,), (1,)), ((), ())), preferred_element_type=F32)


def position(count):
    place = lax.rem(lax.axis_index("tile") + TILES_X // 2, count)
    col, row = lax.rem(place, TILES_X), lax.div(place, TILES_X)
    flag = lambda v: v.astype(jnp.int32)
    return (
        flag(row > 0), flag(row < count // TILES_X - 1), flag(col > 0), flag(col < TILES_X - 1),
        lax.rem(col, 2), lax.rem(row, 2),
    )


def sides(flags):
    top, bottom, left, right, odd = flags[:5]
    as_f = lambda v: v.astype(F32)
    return (
        as_f(top),
        as_f(bottom),
        (as_f(left * odd), as_f(left * (1 - odd))),
        (as_f(right * (1 - odd)), as_f(right * odd)),
    )


def pack_kernel(count, row_pairs, feats_hbm, old1_hbm, old2_hbm, old3_hbm, *refs):
    *outs, feats, old1, old2, old3, near3, far3, sems = refs
    wide3 = old3_hbm.shape[2]
    copies = [
        pltpu.make_async_copy(src, dst, sems.at[i])
        for i, (src, dst) in enumerate((
            (feats_hbm, feats), (old1_hbm, old1), (old2_hbm, old2),
            (old3_hbm.at[:, pl.ds(0, 1)], old3.at[:, pl.ds(0, 1)]),
            (old3_hbm.at[:, pl.ds(old3_hbm.shape[1] - 1, 1)], old3.at[:, pl.ds(1, 1)]),
            (old3_hbm.at[:, :, pl.ds(0, 8)], near3),
            (old3_hbm.at[:, :, pl.ds(wide3 - 8, 8)], far3),
        ))
    ]
    for copy in copies:
        copy.start()
    *_, odd_col, odd_row = position(count)
    for copy in copies:
        copy.wait()
    firsts = [old1.at[f] for f in range(old1.shape[0])] + [feats.at[f] for f in range(feats.shape[0])]
    _, height, width, _ = feats.shape
    c2, c3 = old2.shape[-1], old3.shape[-1]
    aside = slice(256, 256 + c3)
    total = len(firsts)
    outs = list(outs)
    sides_out = {0: outs.pop(0), 1: outs.pop(0)}
    for rp in row_pairs:
        rows2, rows1 = outs.pop(0), outs.pop(0)
        low = odd_row if rp else 1 - odd_row
        start1, start2, start3 = low * (height - 2), low * (2 * height - 2), low
        for i, ref in enumerate(firsts):
            rows1[i] = ref[pl.ds(start1, 2)]
        half = 2 * width
        for f in range(old2.shape[0]):
            rows2[f, :, :, 0:c2] = old2[f, pl.ds(start2, 2)]
            for j in range(2):
                rows2[f, j, :, aside] = old3[f, start3, j * half:(j + 1) * half, :]
        for cp in (0, 1):
            corner = outs.pop(0)
            far = odd_col if cp else 1 - odd_col
            for value in (0, 1):
                @pl.when(far == value)
                def _():
                    pick = lambda n, size: slice(value * (n - size), value * (n - size) + size)
                    for i, ref in enumerate(firsts):
                        corner[2 * i:2 * i + 2] = ref[pl.ds(start1, 2), pick(width, 2), :]
                    for f in range(old2.shape[0]):
                        at = 2 * total + 2 * f
                        corner[at:at + 2, :, 0:c2] = old2[f, pl.ds(start2, 2), pick(2 * width, 2), :]
                        corner[at, 0:1, aside] = old3[f, start3, pick(wide3, 1), :]
    for cp in (0, 1):
        side = sides_out[cp]
        far = odd_col if cp else 1 - odd_col
        for value in (0, 1):
            @pl.when(far == value)
            def _():
                pick = lambda n, size: slice(value * (n - size), value * (n - size) + size)
                for i, ref in enumerate(firsts):
                    side[height * i:height * (i + 1)] = ref[:, pick(width, 2), :]
                for f in range(old2.shape[0]):
                    at = height * total + 2 * height * f
                    side[at:at + 2 * height, :, 0:c2] = old2[f, :, pick(2 * width, 2), :]
                    for r in range(2 * height):
                        ends = near3 if value == 0 else far3
                        pair = [ends[f, 2 * r + j, pick(8, 1), :].astype(F32) for j in range(2)]
                        side[at + r, :, aside] = jnp.concatenate(pair, 0).astype(BF16)


def tap_codes(rows, lanes, rgb, later):
    row = lax.broadcasted_iota(jnp.int32, (rows, lanes), 0)
    lane = lax.broadcasted_iota(jnp.int32, (rows, lanes), 1)
    a, colour, b, time = row % 4, row // 4 % 4, row // 16 % 4, later - row // 64
    c, e, d, t = lane % rgb, lane // rgb % 3, lane // (3 * rgb) % 3, lane // (9 * rgb)
    same = (c == colour) & (t == time)
    return jnp.where(same, a + d, -99), jnp.where(same, b + e, -99)


def tap_weights(w3, wc3, w3c, flat):
    rgb, c3 = w3.shape[3:]
    flat[...] = jnp.zeros_like(flat)
    for t in range(3):
        for d in range(3):
            for e in range(3):
                row = ((t * 3 + d) * 3 + e) * rgb
                flat[row:row + rgb, 0:c3] = w3[t, d, e].astype(F32)
    taps = flat[...].astype(BF16)
    one = lambda cond: jnp.where(cond, 1.0, 0.0).astype(BF16)
    down, over = tap_codes(128, 128, rgb, 1)
    code = down * 8 + over
    for j in range(6):
        for k in range(6):
            base = (j * 6 + k) * 128
            w3c[base:base + 128] = jnp.dot(one(code == j * 8 + k), taps, preferred_element_type=F32).astype(BF16)
    down, over = tap_codes(192, 128, rgb, 2)
    code = ((down + 1) // 2) * 8 + (over + 1) // 2
    lanes = wc3.shape[-1]
    wc3[:, 2 * c3:lanes] = jnp.zeros((wc3.shape[0], lanes - 2 * c3), BF16)
    for rs in range(2):
        for cs in range(4):
            base = (rs * 4 + cs) * 192
            for half in range(2):
                place = {(0, 1): 0, (0, 0): 1, (1, 1): 2, (1, 0): 3}[rs, half]
                value = jnp.dot(one(code == place * 8 + cs), taps, preferred_element_type=F32)
                wc3[base:base + 192, half * c3:(half + 1) * c3] = value[:, 0:c3].astype(BF16)


def phase_weights(w2, wc2):
    c3 = w2.shape[3]
    for t in range(3):
        rows = {}
        for e in range(3):
            w = [w2[t, d, e].astype(F32) for d in range(3)]
            rows[e] = (w[0], w[0] + w[1], w[1] + w[2], w[2])
        for q in range(2):
            for cs in range(2):
                cols = [
                    rows[0][v] if (q, cs) == (0, 0) else rows[2][v] if (q, cs) == (1, 1)
                    else rows[1][v] + (rows[2][v] if q == 0 else rows[0][v])
                    for v in range(4)
                ]
                for rs in range(2):
                    base = ((t * 2 + q) * 2 + rs) * 2 + cs
                    wc2[base, 0:c3, 0:2 * c3] = cols[2 * rs].astype(BF16)
                    wc2[base, c3:2 * c3, 0:2 * c3] = cols[2 * rs + 1].astype(BF16)
    lanes = wc2.shape[-1]
    wc2[:, :, 2 * c3:lanes] = jnp.zeros(wc2.shape[:2] + (lanes - 2 * c3,), BF16)


def weights_kernel(w1_hbm, w2_hbm, w3, w1, w2, wc2, wc3, w3c, flat, sems):
    copies = [
        pltpu.make_async_copy(src, dst, sems.at[i])
        for i, (src, dst) in enumerate(((w2_hbm, w2), (w1_hbm, w1)))
    ]
    for copy in copies:
        copy.start()
    tap_weights(w3, wc3, w3c, flat)
    copies[0].wait()
    phase_weights(w2, wc2)
    copies[1].wait()


def history_kernel(
    count, second, third, up2, down2, side_a, side_b, dau, dbu, dad, dbd, w2, w3c,
    part2, part3,
    e_lo, e_hi, e3, xc2, xc3,
):
    top, bottom, left, right = sides(position(count))
    frames, tall, wide, chans = second.shape
    c3 = third.shape[-1]
    lo = 128
    hi = chans - lo
    read = lambda ref, *ix: ref[ix].astype(F32)
    skip = side_a.shape[0] - frames * tall
    skip_corner = dau.shape[0] - frames * 2
    at_side = lambda ref, f, r: read(ref, skip + f * tall + r)
    at_corner = lambda ref, f, r: read(ref, skip_corner + 2 * f + r)

    off = 8

    def put2(f, row, col, value):
        n = value.shape[0]
        e_lo[f, row, col:col + n, :] = value[:, :lo]
        e_hi[f, row, col:col + n, 0:hi] = value[:, lo:chans]

    for f in range(frames):
        for r in range(tall + 4):
            if r < 2:
                own = read(up2, f, r) * top
                pa, pb, s = at_corner(dau, f, r), at_corner(dbu, f, r), top
            elif r < tall + 2:
                own = read(second, f, r - 2)
                pa, pb, s = at_side(side_a, f, r - 2), at_side(side_b, f, r - 2), 1.0
            else:
                own = read(down2, f, r - tall - 2) * bottom
                pa, pb, s = at_corner(dad, f, r - tall - 2), at_corner(dbd, f, r - tall - 2), bottom
            put2(f, r, off, own)
            put2(f, r, off - 2, pa * (left[0] * s) + pb * (left[1] * s))
            put2(f, r, off + wide, pa * (right[0] * s) + pb * (right[1] * s))
    for k in range(4):
        for f in range(frames):
            for r in range(tall + 4):
                cols = pl.ds(off - 3 + k, PITCH, stride=2)
                xc2[k, f, r, :, 0:lo] = e_lo[f, r, cols, :].astype(BF16)
                xc2[k, f, r, :, lo:chans] = e_hi[f, r, cols, :].astype(BF16)[:, :hi]
    rows_out = tall + 2
    for q in range(2):
        acc = None
        for d in range(3):
            for e in range(3):
                lhs = xc2[e + q, :, d:d + rows_out].reshape(frames * rows_out * PITCH, chans)
                rhs = jnp.concatenate([w2[1, d, e], w2[0, d, e]], 0)
                term = dot_nt(lhs, rhs)
                acc = term if acc is None else acc + term
        acc = acc.reshape(frames, rows_out // 2, 2, PITCH, 2 * c3)
        v0 = acc[0, ..., c3:] + acc[1, ..., :c3]
        v1 = acc[1, ..., c3:]
        for o, v in enumerate((v0, v1)):
            part2[q, o] = jnp.concatenate([v[:, 1], v[:, 0]], -1)

    tall3, wide3 = third.shape[1:3]
    shift = 2 * 128

    def put3(f, row, col, value):
        n = value.shape[0]
        e3[f, row, col:col + n, 0:c3] = value

    for f in range(frames):
        for r in range(tall3):
            put3(f, r + 1, off, read(third, f, r))
        for j in range(2):
            half = wide3 // 2
            put3(f, 0, off + j * half, read(up2, f, j)[:, shift:shift + c3] * top)
            put3(f, tall3 + 1, off + j * half, read(down2, f, j)[:, shift:shift + c3] * bottom)
        for r in range(tall3 // 2):
            pa = at_side(side_a, f, r)[:, shift:shift + c3]
            pb = at_side(side_b, f, r)[:, shift:shift + c3]
            vl = pa * left[0] + pb * left[1]
            vr = pa * right[0] + pb * right[1]
            for j in range(2):
                put3(f, 1 + 2 * r + j, off - 1, vl[j:j + 1])
                put3(f, 1 + 2 * r + j, off + wide3, vr[j:j + 1])
        for row, da, db, s in ((0, dau, dbu, top), (tall3 + 1, dad, dbd, bottom)):
            pa = at_corner(da, f, 0)[0:1, shift:shift + c3]
            pb = at_corner(db, f, 0)[0:1, shift:shift + c3]
            put3(f, row, off - 1, pa * (left[0] * s) + pb * (left[1] * s))
            put3(f, row, off + wide3, pa * (right[0] * s) + pb * (right[1] * s))
    height, width = tall3 // 4, wide3 // 4
    lanes = lax.broadcasted_iota(jnp.int32, (width, 128), 1)
    for k in range(6):
        for f in range(frames):
            for r in range(tall3 + 2):
                value = e3[f, r, pl.ds(off - 1 + k, width, stride=4), :]
                xc3[k, f, r // 4, r % 4] = jnp.where(lanes < c3, value, 0.0).astype(BF16)
    acc = None
    for j in range(6):
        for k in range(0, 6, 2):
            lhs = jnp.concatenate(
                [
                    xc3[kk, :, j // 4:j // 4 + height, j % 4].reshape(frames * height * width, 128)
                    for kk in (k, k + 1)
                ],
                -1,
            )
            base = (j * 6 + k) * 128
            rhs = jnp.concatenate([w3c[base:base + 128], w3c[base + 128:base + 256]], -1)
            term = dot_nt(lhs, rhs)
            acc = term if acc is None else acc + term
    size = height * width
    part3[0] = acc[:size, 64:] + acc[size:, :64]
    part3[1] = acc[size:, 64:]


def normed(values, gain, total):
    meansq = jnp.sum(values * values, axis=-1, keepdims=True) * (1.0 / total)
    out = values * lax.rsqrt(meansq + EPS) * gain
    return out / (1.0 + jnp.exp(-out))


def insides(flags, width, chans):
    cols = lax.broadcasted_iota(jnp.int32, (PITCH, chans), 0)
    first = 1 - flags[2]
    last = width + flags[3]
    inside = (cols >= first) & (cols <= last)
    at_top = inside & (cols < flags[0] * PITCH)
    at_bottom = inside & (cols < flags[1] * PITCH)
    return inside, at_top, at_bottom


def first_kernel(
    count, feats, cache, up1, down1, side_a, side_b, dau, dbu, dad, dbd, w1, g1, g2,
    x2,
    e1, x1, e2,
):
    flags = position(count)
    top, bottom, left, right = sides(flags)
    frames, height, width, chans = feats.shape
    old = cache.shape[0]
    total = frames + old
    c2 = g2.shape[0]
    read = lambda ref, *ix: ref[ix].astype(F32)

    off = 8
    rows1 = height + 2
    lanes2 = e2.shape[-1]
    always = flags[2] + flags[3] > 0
    inside, at_top, at_bottom = insides(flags, width, c2)

    @pl.when(always)
    def _():
        for f in range(total):
            for r in range(height + 4):
                if r < 2:
                    own = read(up1, f, r) * top
                    pa, pb, s = read(dau, 2 * f + r), read(dbu, 2 * f + r), top
                elif r < height + 2:
                    own = read(cache, f, r - 2) if f < old else read(feats, f - old, r - 2)
                    pa, pb, s = read(side_a, f * height + r - 2), read(side_b, f * height + r - 2), 1.0
                else:
                    own = read(down1, f, r - height - 2) * bottom
                    at = 2 * f + r - height - 2
                    pa, pb, s = read(dad, at), read(dbd, at), bottom
                e1[f, r, off:off + width, :] = own
                e1[f, r, off - 2:off, :] = pa * (left[0] * s) + pb * (left[1] * s)
                e1[f, r, off + width:off + width + 2, :] = pa * (right[0] * s) + pb * (right[1] * s)
        gain = g1[...].reshape(1, chans)
        for f in range(old, total):
            for r in range(height + 4):
                e1[f, r] = normed(e1[f, r], gain, chans)
        for k in range(3):
            for f in range(total):
                for r in range(height + 4):
                    x1[k, f, r] = e1[f, r, off - 2 + k:off - 2 + k + PITCH, :].astype(BF16)
        pieces = [
            (t, d, e, slice(i, i + 128))
            for t in range(3) for d in range(3) for e in range(3) for i in range(0, chans, 128)
        ]
        half = frames // 2
        accs = [None, None]
        for i in range(0, len(pieces), 4):
            rhs = jnp.concatenate([w1[t, d, e, :, ch] for t, d, e, ch in pieces[i:i + 4]], -1)
            for h in range(2):
                lhs = [
                    x1[e, t + h * half:t + h * half + half, d:d + rows1, :, ch].reshape(-1, 128)
                    for t, d, e, ch in pieces[i:i + 4]
                ]
                term = dot_nt(jnp.concatenate(lhs, -1), rhs)
                accs[h] = term if accs[h] is None else accs[h] + term
        accs = [v.reshape(half, rows1, PITCH, c2) for v in accs]

        gain = g2[...].reshape(1, c2)
        e2[:, :, :, c2:lanes2] = jnp.zeros(e2.shape[:3] + (lanes2 - c2,), F32)
        for f in range(frames):
            for r in range(rows1):
                keep = at_top if r == 0 else at_bottom if r == rows1 - 1 else inside
                value = jnp.where(keep, accs[f // half][f % half, r].astype(BF16).astype(F32), 0.0)
                e2[f, r, off:off + PITCH, 0:c2] = normed(value, gain, c2)
        for k in range(3):
            for f in range(frames):
                for r in range(rows1):
                    x2[k, f, r] = e2[f, r, off - 1 + k:off - 1 + k + PITCH, :].astype(BF16)


def last_kernel(
    count, x2, g3, part2, part3, wc2, wc3,
    out,
    e2, x3,
):
    flags = position(count)
    frames, rows1 = x2.shape[1:3]
    height = rows1 - 2
    width = out.shape[3] // 4
    c3 = g3.shape[0]
    c2 = 2 * c3
    off = 8
    rows2 = height + 1
    lanes2 = e2.shape[-1]
    always = flags[2] + flags[3] > 0
    inside, at_top, at_bottom = insides(flags, width, c2)
    e2[:, :, :, c2:lanes2] = jnp.zeros(e2.shape[:3] + (lanes2 - c2,), F32)

    @pl.when(always)
    def _():
        lanes = lax.broadcasted_iota(jnp.int32, (PITCH, c2), 1)
        lower = lanes < c3
        gain = jnp.concatenate([g3[...].reshape(1, c3)] * 2, -1)
        every = []
        for q in range(2):
            parts = []
            for t in range(3):
                count = frames - (2 - t)
                acc = None
                for rs in range(2):
                    lhs = [
                        x2[q + cs, 0:count, rs:rs + rows2].reshape(count * rows2 * PITCH, lanes2)
                        for cs in range(2)
                    ]
                    base = ((t * 2 + q) * 2 + rs) * 2
                    term = dot_nt(jnp.concatenate(lhs, -1), jnp.concatenate([wc2[base], wc2[base + 1]], -1))
                    acc = term if acc is None else acc + term
                parts.append(acc.reshape(count, rows2, PITCH, c2))
            every.append(parts)
        for q in range(2):
            parts = every[q]
            for f in range(frames):
                for r in range(rows2):
                    value = parts[2][f, r]
                    if f >= 1:
                        value = value + parts[1][f - 1, r]
                    if f >= 2:
                        value = value + parts[0][f - 2, r]
                    else:
                        value = value + part2[q, f, r]
                    keep = inside
                    if r == 0:
                        keep = (lower & inside) | at_top
                    if r == rows2 - 1:
                        keep = (~lower & inside) | at_bottom
                    value = jnp.where(keep, value.astype(BF16).astype(F32), 0.0)
                    square = value * value
                    sum_low = jnp.sum(jnp.where(lower, square, 0.0), axis=-1, keepdims=True)
                    sum_high = jnp.sum(jnp.where(lower, 0.0, square), axis=-1, keepdims=True)
                    scale = jnp.where(
                        lower,
                        lax.rsqrt(sum_low * (1.0 / c3) + EPS),
                        lax.rsqrt(sum_high * (1.0 / c3) + EPS),
                    )
                    value = value * scale * gain
                    e2[f, r, off:off + PITCH, 0:c2] = value / (1.0 + jnp.exp(-value))
            for f in range(frames):
                for r in range(rows2):
                    for cs in ((1, 3) if q == 0 else (0, 2)):
                        start = off + (0, 1, 1, 2)[cs]
                        x3[cs, f, r] = e2[f, r, start:start + width, :].astype(BF16)

    @pl.when(always)
    def _():
        acc = None
        for rs in range(2):
            for cs in (0, 2):
                lhs = [
                    x3[i, :, rs:rs + height].reshape(frames * height * width, lanes2) for i in (cs, cs + 1)
                ]
                base = (rs * 4 + cs) * 192
                rhs = [wc3[base:base + 192], wc3[base + 192:base + 384]]
                term = dot_nt(jnp.concatenate(lhs, -1), jnp.concatenate(rhs, -1))
                acc = term if acc is None else acc + term
        size = height * width
        acc = acc.reshape(frames, size, 192)
        turned = []
        for f in range(frames):
            value = acc[f, :, 0:64]
            if f >= 1:
                value = value + acc[f - 1, :, 64:128]
            value = value + (acc[f - 2, :, 128:192] if f >= 2 else part3[f])
            value = value.T
            turned.append(jnp.concatenate([value[b * 16:(b + 1) * 16] for b in range(4)], -1))
        turned = jnp.concatenate(turned, 0)
        row = lax.broadcasted_iota(jnp.int32, (4 * size, 4 * size), 0)
        lane = lax.broadcasted_iota(jnp.int32, (4 * size, 4 * size), 1)
        place = row % size * 4 + row // size
        spread = jnp.where(place == lane, 1.0, 0.0).astype(BF16)
        result = None
        for _ in range(3):
            piece = turned.astype(BF16)
            turned = turned - piece.astype(F32)
            term = jnp.dot(piece, spread, preferred_element_type=F32)
            result = term if result is None else result + term
        for f in range(frames):
            for c in range(out.shape[1]):
                for r in range(height):
                    out[f, c, 4 * r:4 * r + 4, :] = result[
                        f * 16 + c * 4:f * 16 + c * 4 + 4, r * 4 * width:(r + 1) * 4 * width
                    ]


def body(count, features, cache_first, cache_second, cache_third, w1, w2, w3, g1, g2, g3):
    tile_rows = count // TILES_X
    last_dims = lambda v: v[:, :, 0].transpose(0, 2, 3, 1)
    feats, old1, old2, old3 = map(last_dims, (features, cache_first, cache_second, cache_third))
    frames, height, width, c1 = feats.shape
    old = old1.shape[0]
    total = frames + old
    c2, c3 = old2.shape[-1], old3.shape[-1]
    rgb = w3.shape[3]
    row_pairs = [0] if tile_rows <= 2 else [0, 1]
    vmem = pl.BlockSpec(memory_space=pltpu.VMEM)
    bf = lambda *shape: jax.ShapeDtypeStruct(shape, BF16)

    def call(kernel, ins, outs, scratch, limit, flops, far=()):
        fn = pl.pallas_call(
            kernel,
            out_shape=outs,
            in_specs=[pl.BlockSpec(memory_space=pltpu.HBM) if i in far else vmem for i in range(len(ins))],
            out_specs=[vmem] * len(outs),
            scratch_shapes=scratch,
            compiler_params=pltpu.CompilerParams(vmem_limit_bytes=int(limit * 2**20)),
            cost_estimate=pl.CostEstimate(flops=flops, bytes_accessed=2_000_000, transcendentals=0),
        )
        ins = [pltpu.with_memory_space_constraint(v, pltpu.HBM) if i in far else v for i, v in enumerate(ins)]
        return fn(*ins)

    side = bf(total * height + old * 2 * height, 2, c1)
    corner = bf(total * 2 + old * 2, 2, c1)
    rows = [bf(old, 2, 2 * width, c1), bf(total, 2, width, c1)]
    packed = call(
        functools.partial(pack_kernel, count, row_pairs), (feats, old1, old2, old3),
        [side] * 2 + (rows + [corner] * 2) * len(row_pairs),
        [
            pltpu.VMEM(feats.shape, BF16),
            pltpu.VMEM(old1.shape, BF16),
            pltpu.VMEM(old2.shape, BF16),
            pltpu.VMEM((old, 2, 4 * width, c3), BF16),
            pltpu.VMEM((old, 4 * height, 8, c3), BF16),
            pltpu.VMEM((old, 4 * height, 8, c3), BF16),
            pltpu.SemaphoreType.DMA((7,)),
        ],
        8, 100_000_000, range(4),
    )

    sent = [swap(packed[cp], count, None, cp) for cp in (0, 1)]
    rows1, rows2, corners = [], [], ([], [])
    for i, rp in enumerate(row_pairs):
        piece = packed[2 + 4 * i:6 + 4 * i]
        rows2.append(swap(piece[0], count, rp, None))
        for cp in (0, 1):
            corners[cp].append(swap(piece[2 + cp], count, rp, cp))
        rows1.append(swap(piece[1], count, rp, None))
    odd_row = (lax.axis_index("tile") + TILES_X // 2) // TILES_X % 2 == 1

    def above(pieces):
        return pieces[0] if len(pieces) == 1 else jnp.where(odd_row, pieces[0], pieces[1])

    def below(pieces):
        return pieces[0] if len(pieces) == 1 else jnp.where(odd_row, pieces[1], pieces[0])

    diagonals = [pick(corners[cp]) for pick in (above, below) for cp in (0, 1)]
    size = height * width
    w1, w2, wc2, wc3, w3c = call(
        weights_kernel, (w1, w2, w3),
        [bf(*w1.shape), bf(*w2.shape), bf(24, 2 * c3, 256), bf(8 * 192, 256), bf(36 * 128, 128)],
        [pltpu.VMEM((128, 128), F32), pltpu.SemaphoreType.DMA((2,))], 16, 500_000_000, (0, 1),
    )
    (x2,) = call(
        functools.partial(first_kernel, count),
        (feats, old1, above(rows1), below(rows1), *sent, *diagonals, w1, g1, g2),
        [bf(3, frames, height + 2, PITCH, 256)],
        [
            pltpu.VMEM((total, height + 4, 40, c1), F32),
            pltpu.VMEM((3, total, height + 4, PITCH, c1), BF16),
            pltpu.VMEM((frames, height + 2, 40, 256), F32),
        ],
        20, 6_000_000_000,
    )
    part2, part3 = call(
        functools.partial(history_kernel, count),
        (old2, old3, above(rows2), below(rows2), *sent, *diagonals, w2, w3c),
        [
            jax.ShapeDtypeStruct((2, 2, height + 1, PITCH, c2), F32),
            jax.ShapeDtypeStruct((2, size, 64), F32),
        ],
        [
            pltpu.VMEM((old, 2 * height + 4, 64, 128), F32),
            pltpu.VMEM((old, 2 * height + 4, 64, 128), F32),
            pltpu.VMEM((old, 4 * height + 2, 96, 128), F32),
            pltpu.VMEM((4, old, 2 * height + 4, PITCH, c2), BF16),
            pltpu.VMEM((6, old, height + 1, 4, width, 128), BF16),
        ],
        22, 4_000_000_000,
    )
    (out,) = call(
        functools.partial(last_kernel, count),
        (x2, g3, part2, part3, wc2, wc3),
        [jax.ShapeDtypeStruct((frames, rgb, 4 * height, 4 * width), F32)],
        [
            pltpu.VMEM((frames, height + 2, 40, 256), F32),
            pltpu.VMEM((4, frames, height + 1, width, 256), BF16),
        ],
        16, 4_000_000_000,
    )
    return out[:, :, None]


def solution(mesh):
    tiled = P("groups", None, "tile", None, None)
    return jax.shard_map(
        functools.partial(body, mesh.shape["tile"]),
        mesh=mesh,
        in_specs=(tiled,) * 4 + (P(),) * 6,
        out_specs=tiled,
        check_vma=False,
    )
```

```python
import functools

import jax
import jax.numpy as jnp
from jax import lax
from jax.experimental import pallas as pl
from jax.experimental.pallas import tpu as pltpu
from jax.sharding import PartitionSpec as P


TILES_X = 8
EPS = 1e-06
F32 = jnp.float32
BF16 = jnp.bfloat16
PITCH = 24
PAIR = 40


def partner(index, size, odd):
    other = index ^ 1 if not odd else ((index - 1) ^ 1) + 1
    return other if 0 <= other < size and (not odd or index > 0) else index


def pairs_of(count, row_pair, col_pair):
    rows = count // TILES_X
    out = []
    for k in range(count):
        m = (k + TILES_X // 2) % count
        r, c = divmod(m, TILES_X)
        r2 = r if row_pair is None else partner(r, rows, row_pair)
        c2 = c if col_pair is None else partner(c, TILES_X, col_pair)
        if (row_pair is not None and r2 == r) or (col_pair is not None and c2 == c):
            r2, c2 = r, c
        out.append((k, (r2 * TILES_X + c2 - TILES_X // 2) % count))
    return out


def swap(values, count, row_pair, col_pair):
    return lax.ppermute(values, "tile", pairs_of(count, row_pair, col_pair))


def dot_nt(lhs, rhs):
    return lax.dot_general(lhs, rhs, (((1,), (1,)), ((), ())), preferred_element_type=F32)


def position(count):
    place = lax.rem(lax.axis_index("tile") + TILES_X // 2, count)
    col, row = lax.rem(place, TILES_X), lax.div(place, TILES_X)
    flag = lambda v: v.astype(jnp.int32)
    return (
        flag(row > 0), flag(row < count // TILES_X - 1), flag(col > 0), flag(col < TILES_X - 1),
        lax.rem(col, 2), lax.rem(row, 2),
    )


def sides(flags):
    top, bottom, left, right, odd = flags[:5]
    as_f = lambda v: v.astype(F32)
    return (
        as_f(top),
        as_f(bottom),
        (as_f(left * odd), as_f(left * (1 - odd))),
        (as_f(right * (1 - odd)), as_f(right * odd)),
    )


def pack_kernel(count, row_pairs, feats_hbm, old1_hbm, old2_hbm, old3_hbm, *refs):
    *outs, feats, old1, old2, old3, near3, far3, sems = refs
    wide3 = old3_hbm.shape[2]
    copies = [
        pltpu.make_async_copy(src, dst, sems.at[i])
        for i, (src, dst) in enumerate((
            (feats_hbm, feats), (old1_hbm, old1), (old2_hbm, old2),
            (old3_hbm.at[:, pl.ds(0, 1)], old3.at[:, pl.ds(0, 1)]),
            (old3_hbm.at[:, pl.ds(old3_hbm.shape[1] - 1, 1)], old3.at[:, pl.ds(1, 1)]),
            (old3_hbm.at[:, :, pl.ds(0, 8)], near3),
            (old3_hbm.at[:, :, pl.ds(wide3 - 8, 8)], far3),
        ))
    ]
    for copy in copies:
        copy.start()
    *_, odd_col, odd_row = position(count)
    for copy in copies:
        copy.wait()
    firsts = [old1.at[f] for f in range(old1.shape[0])] + [feats.at[f] for f in range(feats.shape[0])]
    _, height, width, _ = feats.shape
    c2, c3 = old2.shape[-1], old3.shape[-1]
    aside = slice(256, 256 + c3)
    total = len(firsts)
    outs = list(outs)
    sides_out = {0: outs.pop(0), 1: outs.pop(0)}
    for rp in row_pairs:
        rows2, rows1 = outs.pop(0), outs.pop(0)
        low = odd_row if rp else 1 - odd_row
        start1, start2, start3 = low * (height - 2), low * (2 * height - 2), low
        for i, ref in enumerate(firsts):
            rows1[i] = ref[pl.ds(start1, 2)]
        half = 2 * width
        for f in range(old2.shape[0]):
            rows2[f, :, :, 0:c2] = old2[f, pl.ds(start2, 2)]
            for j in range(2):
                rows2[f, j, :, aside] = old3[f, start3, j * half:(j + 1) * half, :]
        for cp in (0, 1):
            corner = outs.pop(0)
            far = odd_col if cp else 1 - odd_col
            for value in (0, 1):
                @pl.when(far == value)
                def _():
                    pick = lambda n, size: slice(value * (n - size), value * (n - size) + size)
                    for i, ref in enumerate(firsts):
                        corner[2 * i:2 * i + 2] = ref[pl.ds(start1, 2), pick(width, 2), :]
                    for f in range(old2.shape[0]):
                        at = 2 * total + 2 * f
                        corner[at:at + 2, :, 0:c2] = old2[f, pl.ds(start2, 2), pick(2 * width, 2), :]
                        corner[at, 0:1, aside] = old3[f, start3, pick(wide3, 1), :]
    for cp in (0, 1):
        side = sides_out[cp]
        far = odd_col if cp else 1 - odd_col
        for value in (0, 1):
            @pl.when(far == value)
            def _():
                pick = lambda n, size: slice(value * (n - size), value * (n - size) + size)
                for i, ref in enumerate(firsts):
                    side[height * i:height * (i + 1)] = ref[:, pick(width, 2), :]
                for f in range(old2.shape[0]):
                    at = height * total + 2 * height * f
                    side[at:at + 2 * height, :, 0:c2] = old2[f, :, pick(2 * width, 2), :]
                    for r in range(2 * height):
                        ends = near3 if value == 0 else far3
                        pair = [ends[f, 2 * r + j, pick(8, 1), :].astype(F32) for j in range(2)]
                        side[at + r, :, aside] = jnp.concatenate(pair, 0).astype(BF16)


def tap_codes(rows, lanes, rgb, later):
    row = lax.broadcasted_iota(jnp.int32, (rows, lanes), 0)
    lane = lax.broadcasted_iota(jnp.int32, (rows, lanes), 1)
    a, colour, b, time = row % 4, row // 4 % 4, row // 16 % 4, later - row // 64
    c, e, d, t = lane % rgb, lane // rgb % 3, lane // (3 * rgb) % 3, lane // (9 * rgb)
    same = (c == colour) & (t == time)
    return jnp.where(same, a + d, -99), jnp.where(same, b + e, -99)


def tap_weights(w3, wc3, w3c, flat):
    rgb, c3 = w3.shape[3:]
    flat[...] = jnp.zeros_like(flat)
    for t in range(3):
        for d in range(3):
            for e in range(3):
                row = ((t * 3 + d) * 3 + e) * rgb
                flat[row:row + rgb, 0:c3] = w3[t, d, e].astype(F32)
    taps = flat[...].astype(BF16)
    one = lambda cond: jnp.where(cond, 1.0, 0.0).astype(BF16)
    down, over = tap_codes(128, 128, rgb, 1)
    code = down * 8 + over
    for j in range(6):
        for k in range(6):
            base = (j * 6 + k) * 128
            w3c[base:base + 128] = jnp.dot(one(code == j * 8 + k), taps, preferred_element_type=F32).astype(BF16)
    down, over = tap_codes(192, 128, rgb, 2)
    code = ((down + 1) // 2) * 8 + (over + 1) // 2
    lanes = wc3.shape[-1]
    wc3[:, 2 * c3:lanes] = jnp.zeros((wc3.shape[0], lanes - 2 * c3), BF16)
    for rs in range(2):
        for cs in range(4):
            base = (rs * 4 + cs) * 192
            for half in range(2):
                place = {(0, 1): 0, (0, 0): 1, (1, 1): 2, (1, 0): 3}[rs, half]
                value = jnp.dot(one(code == place * 8 + cs), taps, preferred_element_type=F32)
                wc3[base:base + 192, half * c3:(half + 1) * c3] = value[:, 0:c3].astype(BF16)


def phase_weights(w2, wc2):
    c3 = w2.shape[3]
    for t in range(3):
        rows = {}
        for e in range(3):
            w = [w2[t, d, e].astype(F32) for d in range(3)]
            rows[e] = (w[0], w[0] + w[1], w[1] + w[2], w[2])
        for q in range(2):
            for cs in range(2):
                cols = [
                    rows[0][v] if (q, cs) == (0, 0) else rows[2][v] if (q, cs) == (1, 1)
                    else rows[1][v] + (rows[2][v] if q == 0 else rows[0][v])
                    for v in range(4)
                ]
                for rs in range(2):
                    base = ((t * 2 + q) * 2 + rs) * 2 + cs
                    wc2[base, 0:c3, 0:2 * c3] = cols[2 * rs].astype(BF16)
                    wc2[base, c3:2 * c3, 0:2 * c3] = cols[2 * rs + 1].astype(BF16)
    lanes = wc2.shape[-1]
    wc2[:, :, 2 * c3:lanes] = jnp.zeros(wc2.shape[:2] + (lanes - 2 * c3,), BF16)


def weights_kernel(w1_hbm, w2_hbm, w3, w1, w2, wc2, wc3, w3c, flat, sems):
    copies = [
        pltpu.make_async_copy(src, dst, sems.at[i])
        for i, (src, dst) in enumerate(((w2_hbm, w2), (w1_hbm, w1)))
    ]
    for copy in copies:
        copy.start()
    tap_weights(w3, wc3, w3c, flat)
    copies[0].wait()
    phase_weights(w2, wc2)
    copies[1].wait()


def history(
    count, second, third, up2, down2, side_a, side_b, dau, dbu, dad, dbd, w2, w3c,
    part2, part3,
    e_lo, e_hi, e3, xc2, xc3,
):
    top, bottom, left, right = sides(position(count))
    frames, tall, wide, chans = second.shape
    c3 = third.shape[-1]
    lo = 128
    hi = chans - lo
    read = lambda ref, *ix: ref[ix].astype(F32)
    skip = side_a.shape[0] - frames * tall
    skip_corner = dau.shape[0] - frames * 2
    at_side = lambda ref, f, r: read(ref, skip + f * tall + r)
    at_corner = lambda ref, f, r: read(ref, skip_corner + 2 * f + r)

    off = 8

    def put2(f, row, col, value):
        n = value.shape[0]
        e_lo[f, row, col:col + n, :] = value[:, :lo]
        e_hi[f, row, col:col + n, 0:hi] = value[:, lo:chans]

    for f in range(frames):
        for r in range(tall + 4):
            if r < 2:
                own = read(up2, f, r) * top
                pa, pb, s = at_corner(dau, f, r), at_corner(dbu, f, r), top
            elif r < tall + 2:
                own = read(second, f, r - 2)
                pa, pb, s = at_side(side_a, f, r - 2), at_side(side_b, f, r - 2), 1.0
            else:
                own = read(down2, f, r - tall - 2) * bottom
                pa, pb, s = at_corner(dad, f, r - tall - 2), at_corner(dbd, f, r - tall - 2), bottom
            put2(f, r, off, own)
            put2(f, r, off - 2, pa * (left[0] * s) + pb * (left[1] * s))
            put2(f, r, off + wide, pa * (right[0] * s) + pb * (right[1] * s))
    for k in range(4):
        for f in range(frames):
            for r in range(tall + 4):
                cols = pl.ds(off - 3 + k, PITCH, stride=2)
                xc2[k, f, r, :, 0:lo] = e_lo[f, r, cols, :].astype(BF16)
                xc2[k, f, r, :, lo:chans] = e_hi[f, r, cols, :].astype(BF16)[:, :hi]
    rows_out = tall + 2
    for q in range(2):
        acc = None
        for d in range(3):
            for e in range(3):
                lhs = xc2[e + q, :, d:d + rows_out].reshape(frames * rows_out * PITCH, chans)
                rhs = jnp.concatenate([w2[1, d, e], w2[0, d, e]], 0)
                term = dot_nt(lhs, rhs)
                acc = term if acc is None else acc + term
        acc = acc.reshape(frames, rows_out // 2, 2, PITCH, 2 * c3)
        v0 = acc[0, ..., c3:] + acc[1, ..., :c3]
        v1 = acc[1, ..., c3:]
        for o, v in enumerate((v0, v1)):
            part2[q, o] = jnp.concatenate([v[:, 1], v[:, 0]], -1)

    tall3, wide3 = third.shape[1:3]
    shift = 2 * 128

    def put3(f, row, col, value):
        n = value.shape[0]
        e3[f, row, col:col + n, 0:c3] = value

    for f in range(frames):
        for r in range(tall3):
            put3(f, r + 1, off, read(third, f, r))
        for j in range(2):
            half = wide3 // 2
            put3(f, 0, off + j * half, read(up2, f, j)[:, shift:shift + c3] * top)
            put3(f, tall3 + 1, off + j * half, read(down2, f, j)[:, shift:shift + c3] * bottom)
        for r in range(tall3 // 2):
            pa = at_side(side_a, f, r)[:, shift:shift + c3]
            pb = at_side(side_b, f, r)[:, shift:shift + c3]
            vl = pa * left[0] + pb * left[1]
            vr = pa * right[0] + pb * right[1]
            for j in range(2):
                put3(f, 1 + 2 * r + j, off - 1, vl[j:j + 1])
                put3(f, 1 + 2 * r + j, off + wide3, vr[j:j + 1])
        for row, da, db, s in ((0, dau, dbu, top), (tall3 + 1, dad, dbd, bottom)):
            pa = at_corner(da, f, 0)[0:1, shift:shift + c3]
            pb = at_corner(db, f, 0)[0:1, shift:shift + c3]
            put3(f, row, off - 1, pa * (left[0] * s) + pb * (left[1] * s))
            put3(f, row, off + wide3, pa * (right[0] * s) + pb * (right[1] * s))
    height, width = tall3 // 4, wide3 // 4
    lanes = lax.broadcasted_iota(jnp.int32, (width, 128), 1)
    for k in range(6):
        for f in range(frames):
            for r in range(tall3 + 2):
                value = e3[f, r, pl.ds(off - 1 + k, width, stride=4), :]
                xc3[k, f, r // 4, r % 4] = jnp.where(lanes < c3, value, 0.0).astype(BF16)
    acc = None
    for j in range(6):
        for k in range(0, 6, 2):
            lhs = jnp.concatenate(
                [
                    xc3[kk, :, j // 4:j // 4 + height, j % 4].reshape(frames * height * width, 128)
                    for kk in (k, k + 1)
                ],
                -1,
            )
            base = (j * 6 + k) * 128
            rhs = jnp.concatenate([w3c[base:base + 128], w3c[base + 128:base + 256]], -1)
            term = dot_nt(lhs, rhs)
            acc = term if acc is None else acc + term
    size = height * width
    part3[0] = acc[:size, 64:] + acc[size:, :64]
    part3[1] = acc[size:, 64:]


def normed(values, gain, total):
    meansq = jnp.sum(values * values, axis=-1, keepdims=True) * (1.0 / total)
    out = values * lax.rsqrt(meansq + EPS) * gain
    return out / (1.0 + jnp.exp(-out))


def insides(flags, width, chans):
    cols = lax.broadcasted_iota(jnp.int32, (PITCH, chans), 0)
    first = 1 - flags[2]
    last = width + flags[3]
    inside = (cols >= first) & (cols <= last)
    at_top = inside & (cols < flags[0] * PITCH)
    at_bottom = inside & (cols < flags[1] * PITCH)
    return inside, at_top, at_bottom


def first_kernel(
    count, feats, cache, up1, down1, side_a, side_b, dau, dbu, dad, dbd, w1, g1, g2,
    x2,
    e1, x1, e2,
):
    flags = position(count)
    top, bottom, left, right = sides(flags)
    frames, height, width, chans = feats.shape
    old = cache.shape[0]
    total = frames + old
    c2 = g2.shape[0]
    read = lambda ref, *ix: ref[ix].astype(F32)

    off = 8
    rows1 = height + 2
    lanes2 = e2.shape[-1]
    always = flags[2] + flags[3] > 0

    @pl.when(always)
    def _():
        for f in range(total):
            for r in range(height + 4):
                if r < 2:
                    own = read(up1, f, r) * top
                    pa, pb, s = read(dau, 2 * f + r), read(dbu, 2 * f + r), top
                elif r < height + 2:
                    own = read(cache, f, r - 2) if f < old else read(feats, f - old, r - 2)
                    pa, pb, s = read(side_a, f * height + r - 2), read(side_b, f * height + r - 2), 1.0
                else:
                    own = read(down1, f, r - height - 2) * bottom
                    at = 2 * f + r - height - 2
                    pa, pb, s = read(dad, at), read(dbd, at), bottom
                e1[f, r, off:off + width, :] = own
                e1[f, r, off - 2:off, :] = pa * (left[0] * s) + pb * (left[1] * s)
                e1[f, r, off + width:off + width + 2, :] = pa * (right[0] * s) + pb * (right[1] * s)
        gain = g1[...].reshape(1, chans)
        for f in range(old, total):
            for r in range(height + 4):
                e1[f, r] = normed(e1[f, r], gain, chans)
        ringed = width + 2
        for k in range(3):
            for f in range(total):
                for r in range(height + 3):
                    pair = [e1[f, r + i, off - 2 + k:off - 2 + k + ringed, :] for i in range(2)]
                    pair.append(jnp.zeros((PAIR - 2 * ringed, chans), F32))
                    x1[k, f, r % 2, r // 2] = jnp.concatenate(pair, 0).astype(BF16)
        pieces = [
            (t, d, e, slice(i, i + 128))
            for t in range(3) for d in range(3) for e in range(3) for i in range(0, chans, 128)
        ]
        half = frames // 2
        accs = [None, None]
        for i in range(0, len(pieces), 4):
            rhs = jnp.concatenate([w1[t, d, e, :, ch] for t, d, e, ch in pieces[i:i + 4]], -1)
            for h in range(2):
                lhs = [
                    x1[e, t + h * half:t + h * half + half, d % 2, d // 2:d // 2 + rows1 // 2, :, ch].reshape(-1, 128)
                    for t, d, e, ch in pieces[i:i + 4]
                ]
                term = dot_nt(jnp.concatenate(lhs, -1), rhs)
                accs[h] = term if accs[h] is None else accs[h] + term
        accs = [v.reshape(half, rows1 // 2, PAIR, c2) for v in accs]

        gain = g2[...].reshape(1, c2)
        e2[:, :, :, c2:lanes2] = jnp.zeros(e2.shape[:3] + (lanes2 - c2,), F32)
        e2[:, :, 24:e2.shape[2], 0:c2] = jnp.zeros(e2.shape[:2] + (e2.shape[2] - 24, c2), F32)
        spot = lax.broadcasted_iota(jnp.int32, (PAIR, c2), 0)
        upper = spot < ringed
        cols = jnp.where(upper, spot, spot - ringed)
        within = (cols >= 1 - flags[2]) & (cols <= width + flags[3])
        top_pair = within & (~upper | (spot < flags[0] * ringed))
        bottom_pair = within & (upper | (spot < flags[1] * PAIR))
        for f in range(frames):
            for i in range(rows1 // 2):
                keep = top_pair if i == 0 else bottom_pair if i == rows1 // 2 - 1 else within
                value = jnp.where(keep, accs[f // half][f % half, i].astype(BF16).astype(F32), 0.0)
                value = normed(value, gain, c2)
                for j in range(2):
                    e2[f, 2 * i + j, off:off + ringed, 0:c2] = value[j * ringed:(j + 1) * ringed]
        for k in range(3):
            for f in range(frames):
                for r in range(rows1):
                    x2[k, f, r] = e2[f, r, off - 1 + k:off - 1 + k + PITCH, :].astype(BF16)


def last_kernel(
    count, second, third, up2, down2, side_a, side_b, dau, dbu, dad, dbd, w2, w3c, x2, g3, wc2, wc3,
    out,
    part2, part3, e_lo, e_hi, e3, xc2, xc3, e2, x3,
):
    flags = position(count)
    frames, rows1 = x2.shape[1:3]
    height = rows1 - 2
    width = out.shape[3] // 4
    c3 = g3.shape[0]
    c2 = 2 * c3
    off = 8
    rows2 = height + 1
    lanes2 = e2.shape[-1]
    always = flags[2] + flags[3] > 0
    inside, at_top, at_bottom = insides(flags, width, c2)
    e2[:, :, :, c2:lanes2] = jnp.zeros(e2.shape[:3] + (lanes2 - c2,), F32)

    @pl.when(always)
    def _():
        history(
            count, second, third, up2, down2, side_a, side_b, dau, dbu, dad, dbd, w2, w3c,
            part2, part3, e_lo, e_hi, e3, xc2, xc3,
        )
        lanes = lax.broadcasted_iota(jnp.int32, (PITCH, c2), 1)
        lower = lanes < c3
        gain = jnp.concatenate([g3[...].reshape(1, c3)] * 2, -1)
        every = []
        for q in range(2):
            parts = []
            for t in range(3):
                many = frames - (2 - t)
                acc = None
                for rs in range(2):
                    lhs = [
                        x2[q + cs, 0:many, rs:rs + rows2].reshape(many * rows2 * PITCH, lanes2)
                        for cs in range(2)
                    ]
                    base = ((t * 2 + q) * 2 + rs) * 2
                    term = dot_nt(jnp.concatenate(lhs, -1), jnp.concatenate([wc2[base], wc2[base + 1]], -1))
                    acc = term if acc is None else acc + term
                parts.append(acc.reshape(many, rows2, PITCH, c2))
            every.append(parts)
        for q in range(2):
            parts = every[q]
            for f in range(frames):
                for r in range(rows2):
                    value = parts[2][f, r]
                    if f >= 1:
                        value = value + parts[1][f - 1, r]
                    if f >= 2:
                        value = value + parts[0][f - 2, r]
                    else:
                        value = value + part2[q, f, r]
                    keep = inside
                    if r == 0:
                        keep = (lower & inside) | at_top
                    if r == rows2 - 1:
                        keep = (~lower & inside) | at_bottom
                    value = jnp.where(keep, value.astype(BF16).astype(F32), 0.0)
                    square = value * value
                    sum_low = jnp.sum(jnp.where(lower, square, 0.0), axis=-1, keepdims=True)
                    sum_high = jnp.sum(jnp.where(lower, 0.0, square), axis=-1, keepdims=True)
                    scale = jnp.where(
                        lower,
                        lax.rsqrt(sum_low * (1.0 / c3) + EPS),
                        lax.rsqrt(sum_high * (1.0 / c3) + EPS),
                    )
                    value = value * scale * gain
                    e2[f, r, off:off + PITCH, 0:c2] = value / (1.0 + jnp.exp(-value))
            for f in range(frames):
                for r in range(rows2):
                    for cs in ((1, 3) if q == 0 else (0, 2)):
                        start = off + (0, 1, 1, 2)[cs]
                        x3[cs, f, r] = e2[f, r, start:start + width, :].astype(BF16)

    @pl.when(always)
    def _():
        acc = None
        for rs in range(2):
            for cs in (0, 2):
                lhs = [
                    x3[i, :, rs:rs + height].reshape(frames * height * width, lanes2) for i in (cs, cs + 1)
                ]
                base = (rs * 4 + cs) * 192
                rhs = [wc3[base:base + 192], wc3[base + 192:base + 384]]
                term = dot_nt(jnp.concatenate(lhs, -1), jnp.concatenate(rhs, -1))
                acc = term if acc is None else acc + term
        size = height * width
        acc = acc.reshape(frames, size, 192)
        turned = []
        for f in range(frames):
            value = acc[f, :, 0:64]
            if f >= 1:
                value = value + acc[f - 1, :, 64:128]
            value = value + (acc[f - 2, :, 128:192] if f >= 2 else part3[f])
            value = value.T
            turned.append(jnp.concatenate([value[b * 16:(b + 1) * 16] for b in range(4)], -1))
        turned = jnp.concatenate(turned, 0)
        row = lax.broadcasted_iota(jnp.int32, (4 * size, 4 * size), 0)
        lane = lax.broadcasted_iota(jnp.int32, (4 * size, 4 * size), 1)
        place = row % size * 4 + row // size
        spread = jnp.where(place == lane, 1.0, 0.0).astype(BF16)
        result = None
        for _ in range(3):
            piece = turned.astype(BF16)
            turned = turned - piece.astype(F32)
            term = jnp.dot(piece, spread, preferred_element_type=F32)
            result = term if result is None else result + term
        for f in range(frames):
            for c in range(out.shape[1]):
                for r in range(height):
                    out[f, c, 4 * r:4 * r + 4, :] = result[
                        f * 16 + c * 4:f * 16 + c * 4 + 4, r * 4 * width:(r + 1) * 4 * width
                    ]


def body(count, features, cache_first, cache_second, cache_third, w1, w2, w3, g1, g2, g3):
    tile_rows = count // TILES_X
    last_dims = lambda v: v[:, :, 0].transpose(0, 2, 3, 1)
    feats, old1, old2, old3 = map(last_dims, (features, cache_first, cache_second, cache_third))
    frames, height, width, c1 = feats.shape
    old = old1.shape[0]
    total = frames + old
    c2, c3 = old2.shape[-1], old3.shape[-1]
    rgb = w3.shape[3]
    row_pairs = [0] if tile_rows <= 2 else [0, 1]
    vmem = pl.BlockSpec(memory_space=pltpu.VMEM)
    bf = lambda *shape: jax.ShapeDtypeStruct(shape, BF16)

    def call(kernel, ins, outs, scratch, limit, flops, far=()):
        fn = pl.pallas_call(
            kernel,
            out_shape=outs,
            in_specs=[pl.BlockSpec(memory_space=pltpu.HBM) if i in far else vmem for i in range(len(ins))],
            out_specs=[vmem] * len(outs),
            scratch_shapes=scratch,
            compiler_params=pltpu.CompilerParams(vmem_limit_bytes=int(limit * 2**20)),
            cost_estimate=pl.CostEstimate(flops=flops, bytes_accessed=2_000_000, transcendentals=0),
        )
        ins = [pltpu.with_memory_space_constraint(v, pltpu.HBM) if i in far else v for i, v in enumerate(ins)]
        return fn(*ins)

    side = bf(total * height + old * 2 * height, 2, c1)
    corner = bf(total * 2 + old * 2, 2, c1)
    rows = [bf(old, 2, 2 * width, c1), bf(total, 2, width, c1)]
    packed = call(
        functools.partial(pack_kernel, count, row_pairs), (feats, old1, old2, old3),
        [side] * 2 + (rows + [corner] * 2) * len(row_pairs),
        [
            pltpu.VMEM(feats.shape, BF16),
            pltpu.VMEM(old1.shape, BF16),
            pltpu.VMEM(old2.shape, BF16),
            pltpu.VMEM((old, 2, 4 * width, c3), BF16),
            pltpu.VMEM((old, 4 * height, 8, c3), BF16),
            pltpu.VMEM((old, 4 * height, 8, c3), BF16),
            pltpu.SemaphoreType.DMA((7,)),
        ],
        8, 100_000_000, range(4),
    )

    sent = [swap(packed[cp], count, None, cp) for cp in (0, 1)]
    rows1, rows2, corners = [], [], ([], [])
    for i, rp in enumerate(row_pairs):
        piece = packed[2 + 4 * i:6 + 4 * i]
        rows2.append(swap(piece[0], count, rp, None))
        for cp in (0, 1):
            corners[cp].append(swap(piece[2 + cp], count, rp, cp))
        rows1.append(swap(piece[1], count, rp, None))
    odd_row = (lax.axis_index("tile") + TILES_X // 2) // TILES_X % 2 == 1

    def above(pieces):
        return pieces[0] if len(pieces) == 1 else jnp.where(odd_row, pieces[0], pieces[1])

    def below(pieces):
        return pieces[0] if len(pieces) == 1 else jnp.where(odd_row, pieces[1], pieces[0])

    diagonals = [pick(corners[cp]) for pick in (above, below) for cp in (0, 1)]
    size = height * width
    w1, w2, wc2, wc3, w3c = call(
        weights_kernel, (w1, w2, w3),
        [bf(*w1.shape), bf(*w2.shape), bf(24, 2 * c3, 256), bf(8 * 192, 256), bf(36 * 128, 128)],
        [pltpu.VMEM((128, 128), F32), pltpu.SemaphoreType.DMA((2,))], 16, 500_000_000, (0, 1),
    )
    (x2,) = call(
        functools.partial(first_kernel, count),
        (feats, old1, above(rows1), below(rows1), *sent, *diagonals, w1, g1, g2),
        [bf(3, frames, height + 2, PITCH, 256)],
        [
            pltpu.VMEM((total, height + 4, 40, c1), F32),
            pltpu.VMEM((3, total, 2, height // 2 + 2, PAIR, c1), BF16),
            pltpu.VMEM((frames, height + 2, 40, 256), F32),
        ],
        22, 6_000_000_000,
    )
    (out,) = call(
        functools.partial(last_kernel, count),
        (old2, old3, above(rows2), below(rows2), *sent, *diagonals, w2, w3c, x2, g3, wc2, wc3),
        [jax.ShapeDtypeStruct((frames, rgb, 4 * height, 4 * width), F32)],
        [
            pltpu.VMEM((2, 2, height + 1, PITCH, c2), F32),
            pltpu.VMEM((2, size, 64), F32),
            pltpu.VMEM((old, 2 * height + 4, 64, 128), F32),
            pltpu.VMEM((old, 2 * height + 4, 64, 128), F32),
            pltpu.VMEM((old, 4 * height + 2, 96, 128), F32),
            pltpu.VMEM((4, old, 2 * height + 4, PITCH, c2), BF16),
            pltpu.VMEM((6, old, height + 1, 4, width, 128), BF16),
            pltpu.VMEM((frames, height + 2, 40, 256), F32),
            pltpu.VMEM((4, frames, height + 1, width, 256), BF16),
        ],
        30, 8_000_000_000,
    )
    return out[:, :, None]


def solution(mesh):
    tiled = P("groups", None, "tile", None, None)
    return jax.shard_map(
        functools.partial(body, mesh.shape["tile"]),
        mesh=mesh,
        in_specs=(tiled,) * 4 + (P(),) * 6,
        out_specs=tiled,
        check_vma=False,
    )
```

```python
import functools

import jax
import jax.numpy as jnp
from jax import lax
from jax.experimental import pallas as pl
from jax.experimental.pallas import tpu as pltpu
from jax.sharding import PartitionSpec as P


TILES_X = 8
EPS = 1e-06
F32 = jnp.float32
BF16 = jnp.bfloat16
PITCH = 24
PAIR = 40
TRIPLE = 56


def partner(index, size, odd):
    other = index ^ 1 if not odd else ((index - 1) ^ 1) + 1
    return other if 0 <= other < size and (not odd or index > 0) else index


def pairs_of(count, row_pair, col_pair):
    rows = count // TILES_X
    out = []
    for k in range(count):
        m = (k + TILES_X // 2) % count
        r, c = divmod(m, TILES_X)
        r2 = r if row_pair is None else partner(r, rows, row_pair)
        c2 = c if col_pair is None else partner(c, TILES_X, col_pair)
        if (row_pair is not None and r2 == r) or (col_pair is not None and c2 == c):
            r2, c2 = r, c
        out.append((k, (r2 * TILES_X + c2 - TILES_X // 2) % count))
    return out


def swap(values, count, row_pair, col_pair):
    return lax.ppermute(values, "tile", pairs_of(count, row_pair, col_pair))


def dot_nt(lhs, rhs):
    return lax.dot_general(lhs, rhs, (((1,), (1,)), ((), ())), preferred_element_type=F32)


def position(count):
    place = lax.rem(lax.axis_index("tile") + TILES_X // 2, count)
    col, row = lax.rem(place, TILES_X), lax.div(place, TILES_X)
    flag = lambda v: v.astype(jnp.int32)
    return (
        flag(row > 0), flag(row < count // TILES_X - 1), flag(col > 0), flag(col < TILES_X - 1),
        lax.rem(col, 2), lax.rem(row, 2),
    )


def sides(flags):
    top, bottom, left, right, odd = flags[:5]
    as_f = lambda v: v.astype(F32)
    return (
        as_f(top),
        as_f(bottom),
        (as_f(left * odd), as_f(left * (1 - odd))),
        (as_f(right * (1 - odd)), as_f(right * odd)),
    )


def pack_kernel(count, row_pairs, feats_hbm, old1_hbm, old2_hbm, old3_hbm, *refs):
    *outs, feats, old1, old2, old3, near3, far3, sems = refs
    wide3 = old3_hbm.shape[2]
    copies = [
        pltpu.make_async_copy(src, dst, sems.at[i])
        for i, (src, dst) in enumerate((
            (feats_hbm, feats), (old1_hbm, old1), (old2_hbm, old2),
            (old3_hbm.at[:, pl.ds(0, 1)], old3.at[:, pl.ds(0, 1)]),
            (old3_hbm.at[:, pl.ds(old3_hbm.shape[1] - 1, 1)], old3.at[:, pl.ds(1, 1)]),
            (old3_hbm.at[:, :, pl.ds(0, 8)], near3),
            (old3_hbm.at[:, :, pl.ds(wide3 - 8, 8)], far3),
        ))
    ]
    for copy in copies:
        copy.start()
    *_, odd_col, odd_row = position(count)
    for copy in copies:
        copy.wait()
    firsts = [old1.at[f] for f in range(old1.shape[0])] + [feats.at[f] for f in range(feats.shape[0])]
    _, height, width, _ = feats.shape
    c2, c3 = old2.shape[-1], old3.shape[-1]
    aside = slice(256, 256 + c3)
    total = len(firsts)
    outs = list(outs)
    sides_out = {0: outs.pop(0), 1: outs.pop(0)}
    for rp in row_pairs:
        rows2, rows1 = outs.pop(0), outs.pop(0)
        low = odd_row if rp else 1 - odd_row
        start1, start2, start3 = low * (height - 2), low * (2 * height - 2), low
        for i, ref in enumerate(firsts):
            rows1[i] = ref[pl.ds(start1, 2)]
        half = 2 * width
        for f in range(old2.shape[0]):
            rows2[f, :, :, 0:c2] = old2[f, pl.ds(start2, 2)]
            for j in range(2):
                rows2[f, j, :, aside] = old3[f, start3, j * half:(j + 1) * half, :]
        for cp in (0, 1):
            corner = outs.pop(0)
            far = odd_col if cp else 1 - odd_col
            for value in (0, 1):
                @pl.when(far == value)
                def _():
                    pick = lambda n, size: slice(value * (n - size), value * (n - size) + size)
                    for i, ref in enumerate(firsts):
                        corner[2 * i:2 * i + 2] = ref[pl.ds(start1, 2), pick(width, 2), :]
                    for f in range(old2.shape[0]):
                        at = 2 * total + 2 * f
                        corner[at:at + 2, :, 0:c2] = old2[f, pl.ds(start2, 2), pick(2 * width, 2), :]
                        corner[at, 0:1, aside] = old3[f, start3, pick(wide3, 1), :]
    for cp in (0, 1):
        side = sides_out[cp]
        far = odd_col if cp else 1 - odd_col
        for value in (0, 1):
            @pl.when(far == value)
            def _():
                pick = lambda n, size: slice(value * (n - size), value * (n - size) + size)
                for i, ref in enumerate(firsts):
                    side[height * i:height * (i + 1)] = ref[:, pick(width, 2), :]
                for f in range(old2.shape[0]):
                    at = height * total + 2 * height * f
                    side[at:at + 2 * height, :, 0:c2] = old2[f, :, pick(2 * width, 2), :]
                    for r in range(2 * height):
                        ends = near3 if value == 0 else far3
                        pair = [ends[f, 2 * r + j, pick(8, 1), :].astype(F32) for j in range(2)]
                        side[at + r, :, aside] = jnp.concatenate(pair, 0).astype(BF16)


def tap_codes(rows, lanes, rgb, later):
    row = lax.broadcasted_iota(jnp.int32, (rows, lanes), 0)
    lane = lax.broadcasted_iota(jnp.int32, (rows, lanes), 1)
    a, colour, b, time = row % 4, row // 4 % 4, row // 16 % 4, later - row // 64
    c, e, d, t = lane % rgb, lane // rgb % 3, lane // (3 * rgb) % 3, lane // (9 * rgb)
    same = (c == colour) & (t == time)
    return jnp.where(same, a + d, -99), jnp.where(same, b + e, -99)


def tap_weights(w3, wc3, w3c, flat):
    rgb, c3 = w3.shape[3:]
    flat[...] = jnp.zeros_like(flat)
    for t in range(3):
        for d in range(3):
            for e in range(3):
                row = ((t * 3 + d) * 3 + e) * rgb
                flat[row:row + rgb, 0:c3] = w3[t, d, e].astype(F32)
    taps = flat[...].astype(BF16)
    one = lambda cond: jnp.where(cond, 1.0, 0.0).astype(BF16)
    down, over = tap_codes(128, 128, rgb, 1)
    code = down * 8 + over
    for j in range(6):
        for k in range(6):
            base = (j * 6 + k) * 128
            w3c[base:base + 128] = jnp.dot(one(code == j * 8 + k), taps, preferred_element_type=F32).astype(BF16)
    down, over = tap_codes(192, 128, rgb, 2)
    code = ((down + 1) // 2) * 8 + (over + 1) // 2
    lanes = wc3.shape[-1]
    wc3[:, 2 * c3:lanes] = jnp.zeros((wc3.shape[0], lanes - 2 * c3), BF16)
    for rs in range(2):
        for cs in range(4):
            base = (rs * 4 + cs) * 192
            for half in range(2):
                place = {(0, 1): 0, (0, 0): 1, (1, 1): 2, (1, 0): 3}[rs, half]
                value = jnp.dot(one(code == place * 8 + cs), taps, preferred_element_type=F32)
                wc3[base:base + 192, half * c3:(half + 1) * c3] = value[:, 0:c3].astype(BF16)


def phase_weights(w2, wc2):
    c3 = w2.shape[3]
    for t in range(3):
        rows = {}
        for e in range(3):
            w = [w2[t, d, e].astype(F32) for d in range(3)]
            rows[e] = (w[0], w[0] + w[1], w[1] + w[2], w[2])
        for q in range(2):
            for cs in range(2):
                cols = [
                    rows[0][v] if (q, cs) == (0, 0) else rows[2][v] if (q, cs) == (1, 1)
                    else rows[1][v] + (rows[2][v] if q == 0 else rows[0][v])
                    for v in range(4)
                ]
                for rs in range(2):
                    base = ((t * 2 + q) * 2 + rs) * 2 + cs
                    wc2[base, 0:c3, 0:2 * c3] = cols[2 * rs].astype(BF16)
                    wc2[base, c3:2 * c3, 0:2 * c3] = cols[2 * rs + 1].astype(BF16)
    lanes = wc2.shape[-1]
    wc2[:, :, 2 * c3:lanes] = jnp.zeros(wc2.shape[:2] + (lanes - 2 * c3,), BF16)


def weights_kernel(w1_hbm, w2_hbm, w3, w1, w2, wc2, wc3, w3c, flat, sems):
    copies = [
        pltpu.make_async_copy(src, dst, sems.at[i])
        for i, (src, dst) in enumerate(((w2_hbm, w2), (w1_hbm, w1)))
    ]
    for copy in copies:
        copy.start()
    tap_weights(w3, wc3, w3c, flat)
    copies[0].wait()
    phase_weights(w2, wc2)
    copies[1].wait()


def history(
    count, second, third, up2, down2, side_a, side_b, dau, dbu, dad, dbd, w2, w3c,
    part2, part3,
    e_lo, e_hi, e3, xc2, xc3,
):
    top, bottom, left, right = sides(position(count))
    frames, tall, wide, chans = second.shape
    c3 = third.shape[-1]
    lo = 128
    hi = chans - lo
    read = lambda ref, *ix: ref[ix].astype(F32)
    skip = side_a.shape[0] - frames * tall
    skip_corner = dau.shape[0] - frames * 2
    at_side = lambda ref, f, r: read(ref, skip + f * tall + r)
    at_corner = lambda ref, f, r: read(ref, skip_corner + 2 * f + r)

    off = 8

    def put2(f, row, col, value):
        n = value.shape[0]
        e_lo[f, row, col:col + n, :] = value[:, :lo]
        e_hi[f, row, col:col + n, 0:hi] = value[:, lo:chans]

    for f in range(frames):
        for r in range(tall + 4):
            if r < 2:
                own = read(up2, f, r) * top
                pa, pb, s = at_corner(dau, f, r), at_corner(dbu, f, r), top
            elif r < tall + 2:
                own = read(second, f, r - 2)
                pa, pb, s = at_side(side_a, f, r - 2), at_side(side_b, f, r - 2), 1.0
            else:
                own = read(down2, f, r - tall - 2) * bottom
                pa, pb, s = at_corner(dad, f, r - tall - 2), at_corner(dbd, f, r - tall - 2), bottom
            put2(f, r, off, own)
            put2(f, r, off - 2, pa * (left[0] * s) + pb * (left[1] * s))
            put2(f, r, off + wide, pa * (right[0] * s) + pb * (right[1] * s))
    for k in range(4):
        for f in range(frames):
            for r in range(tall + 4):
                cols = pl.ds(off - 3 + k, PITCH, stride=2)
                xc2[k, f, r, :, 0:lo] = e_lo[f, r, cols, :].astype(BF16)
                xc2[k, f, r, :, lo:chans] = e_hi[f, r, cols, :].astype(BF16)[:, :hi]
    rows_out = tall + 2
    for q in range(2):
        acc = None
        for d in range(3):
            for e in range(3):
                lhs = xc2[e + q, :, d:d + rows_out].reshape(frames * rows_out * PITCH, chans)
                rhs = jnp.concatenate([w2[1, d, e], w2[0, d, e]], 0)
                term = dot_nt(lhs, rhs)
                acc = term if acc is None else acc + term
        acc = acc.reshape(frames, rows_out // 2, 2, PITCH, 2 * c3)
        v0 = acc[0, ..., c3:] + acc[1, ..., :c3]
        v1 = acc[1, ..., c3:]
        for o, v in enumerate((v0, v1)):
            both = jnp.concatenate([v[:, 1], v[:, 0]], -1)
            ringed = wide // 2 + 2
            for i in range(part2.shape[2]):
                rows = [both[3 * i + j, :ringed] for j in range(3)]
                rows.append(jnp.zeros((TRIPLE - 3 * ringed, 2 * c3), F32))
                part2[q, o, i] = jnp.concatenate(rows, 0)

    tall3, wide3 = third.shape[1:3]
    shift = 2 * 128

    def put3(f, row, col, value):
        n = value.shape[0]
        e3[f, row, col:col + n, 0:c3] = value

    for f in range(frames):
        for r in range(tall3):
            put3(f, r + 1, off, read(third, f, r))
        for j in range(2):
            half = wide3 // 2
            put3(f, 0, off + j * half, read(up2, f, j)[:, shift:shift + c3] * top)
            put3(f, tall3 + 1, off + j * half, read(down2, f, j)[:, shift:shift + c3] * bottom)
        for r in range(tall3 // 2):
            pa = at_side(side_a, f, r)[:, shift:shift + c3]
            pb = at_side(side_b, f, r)[:, shift:shift + c3]
            vl = pa * left[0] + pb * left[1]
            vr = pa * right[0] + pb * right[1]
            for j in range(2):
                put3(f, 1 + 2 * r + j, off - 1, vl[j:j + 1])
                put3(f, 1 + 2 * r + j, off + wide3, vr[j:j + 1])
        for row, da, db, s in ((0, dau, dbu, top), (tall3 + 1, dad, dbd, bottom)):
            pa = at_corner(da, f, 0)[0:1, shift:shift + c3]
            pb = at_corner(db, f, 0)[0:1, shift:shift + c3]
            put3(f, row, off - 1, pa * (left[0] * s) + pb * (left[1] * s))
            put3(f, row, off + wide3, pa * (right[0] * s) + pb * (right[1] * s))
    height, width = tall3 // 4, wide3 // 4
    lanes = lax.broadcasted_iota(jnp.int32, (width, 128), 1)
    for k in range(6):
        for f in range(frames):
            for r in range(tall3 + 2):
                value = e3[f, r, pl.ds(off - 1 + k, width, stride=4), :]
                xc3[k, f, r // 4, r % 4] = jnp.where(lanes < c3, value, 0.0).astype(BF16)
    acc = None
    for j in range(6):
        for k in range(0, 6, 2):
            lhs = jnp.concatenate(
                [
                    xc3[kk, :, j // 4:j // 4 + height, j % 4].reshape(frames * height * width, 128)
                    for kk in (k, k + 1)
                ],
                -1,
            )
            base = (j * 6 + k) * 128
            rhs = jnp.concatenate([w3c[base:base + 128], w3c[base + 128:base + 256]], -1)
            term = dot_nt(lhs, rhs)
            acc = term if acc is None else acc + term
    size = height * width
    part3[0] = acc[:size, 64:] + acc[size:, :64]
    part3[1] = acc[size:, 64:]


def normed(values, gain, total):
    meansq = jnp.sum(values * values, axis=-1, keepdims=True) * (1.0 / total)
    out = values * lax.rsqrt(meansq + EPS) * gain
    return out / (1.0 + jnp.exp(-out))


def first_kernel(
    count, feats, cache, up1, down1, side_a, side_b, dau, dbu, dad, dbd, w1, g1, g2,
    x2,
    e1, x1, e2,
):
    flags = position(count)
    top, bottom, left, right = sides(flags)
    frames, height, width, chans = feats.shape
    old = cache.shape[0]
    total = frames + old
    c2 = g2.shape[0]
    read = lambda ref, *ix: ref[ix].astype(F32)

    off = 8
    rows1 = height + 2
    lanes2 = e2.shape[-1]
    always = flags[2] + flags[3] > 0

    @pl.when(always)
    def _():
        for f in range(total):
            for r in range(height + 4):
                if r < 2:
                    own = read(up1, f, r) * top
                    pa, pb, s = read(dau, 2 * f + r), read(dbu, 2 * f + r), top
                elif r < height + 2:
                    own = read(cache, f, r - 2) if f < old else read(feats, f - old, r - 2)
                    pa, pb, s = read(side_a, f * height + r - 2), read(side_b, f * height + r - 2), 1.0
                else:
                    own = read(down1, f, r - height - 2) * bottom
                    at = 2 * f + r - height - 2
                    pa, pb, s = read(dad, at), read(dbd, at), bottom
                e1[f, r, off:off + width, :] = own
                e1[f, r, off - 2:off, :] = pa * (left[0] * s) + pb * (left[1] * s)
                e1[f, r, off + width:off + width + 2, :] = pa * (right[0] * s) + pb * (right[1] * s)
        gain = g1[...].reshape(1, chans)
        for f in range(old, total):
            for r in range(height + 4):
                e1[f, r] = normed(e1[f, r], gain, chans)
        ringed = width + 2
        for k in range(3):
            for f in range(total):
                for r in range(height + 3):
                    pair = [e1[f, r + i, off - 2 + k:off - 2 + k + ringed, :] for i in range(2)]
                    pair.append(jnp.zeros((PAIR - 2 * ringed, chans), F32))
                    x1[k, f, r % 2, r // 2] = jnp.concatenate(pair, 0).astype(BF16)
        pieces = [
            (t, d, e, slice(i, i + 128))
            for t in range(3) for d in range(3) for e in range(3) for i in range(0, chans, 128)
        ]
        half = frames // 2
        accs = [None, None]
        for i in range(0, len(pieces), 4):
            rhs = jnp.concatenate([w1[t, d, e, :, ch] for t, d, e, ch in pieces[i:i + 4]], -1)
            for h in range(2):
                lhs = [
                    x1[e, t + h * half:t + h * half + half, d % 2, d // 2:d // 2 + rows1 // 2, :, ch].reshape(-1, 128)
                    for t, d, e, ch in pieces[i:i + 4]
                ]
                term = dot_nt(jnp.concatenate(lhs, -1), rhs)
                accs[h] = term if accs[h] is None else accs[h] + term
        accs = [v.reshape(half, rows1 // 2, PAIR, c2) for v in accs]

        gain = g2[...].reshape(1, c2)
        e2[:, :, :, c2:lanes2] = jnp.zeros(e2.shape[:3] + (lanes2 - c2,), F32)
        e2[:, :, 24:e2.shape[2], 0:c2] = jnp.zeros(e2.shape[:2] + (e2.shape[2] - 24, c2), F32)
        spot = lax.broadcasted_iota(jnp.int32, (PAIR, c2), 0)
        upper = spot < ringed
        cols = jnp.where(upper, spot, spot - ringed)
        within = (cols >= 1 - flags[2]) & (cols <= width + flags[3])
        top_pair = within & (~upper | (spot < flags[0] * ringed))
        bottom_pair = within & (upper | (spot < flags[1] * PAIR))
        for f in range(frames):
            for i in range(rows1 // 2):
                keep = top_pair if i == 0 else bottom_pair if i == rows1 // 2 - 1 else within
                value = jnp.where(keep, accs[f // half][f % half, i].astype(BF16).astype(F32), 0.0)
                value = normed(value, gain, c2)
                for j in range(2):
                    e2[f, 2 * i + j, off:off + ringed, 0:c2] = value[j * ringed:(j + 1) * ringed]
        for k in range(3):
            for f in range(frames):
                for rs in range(2):
                    for i in range(rows1 // 3):
                        rows = [
                            e2[f, rs + 3 * i + j, off - 1 + k:off - 1 + k + ringed, :] for j in range(3)
                        ]
                        rows.append(jnp.zeros((TRIPLE - 3 * ringed, lanes2), F32))
                        x2[k, f, rs, i] = jnp.concatenate(rows, 0).astype(BF16)


def last_kernel(
    count, second, third, up2, down2, side_a, side_b, dau, dbu, dad, dbd, w2, w3c, x2, g3, wc2, wc3,
    out,
    part2, part3, e_lo, e_hi, e3, xc2, xc3, e2, x3,
):
    flags = position(count)
    frames, _, triples = x2.shape[1:4]
    height = 3 * triples - 1
    width = out.shape[3] // 4
    c3 = g3.shape[0]
    c2 = 2 * c3
    off = 8
    rows2 = height + 1
    lanes2 = e2.shape[-1]
    always = flags[2] + flags[3] > 0
    e2[:, :, :, c2:lanes2] = jnp.zeros(e2.shape[:3] + (lanes2 - c2,), F32)

    @pl.when(always)
    def _():
        ringed = width + 2
        lanes = lax.broadcasted_iota(jnp.int32, (TRIPLE, c2), 1)
        spot = lax.broadcasted_iota(jnp.int32, (TRIPLE, c2), 0)
        row = (spot >= ringed).astype(jnp.int32) + (spot >= 2 * ringed).astype(jnp.int32)
        cols = spot - row * ringed
        within = (cols >= 1 - flags[2]) & (cols <= width + flags[3])
        lower = lanes < c3
        gain = jnp.concatenate([g3[...].reshape(1, c3)] * 2, -1)
        every = []
        for q in range(2):
            parts = []
            for t in range(3):
                many = frames - (2 - t)
                acc = None
                for rs in range(2):
                    lhs = [
                        x2[q + cs, 0:many, rs].reshape(many * triples * TRIPLE, lanes2)
                        for cs in range(2)
                    ]
                    base = ((t * 2 + q) * 2 + rs) * 2
                    term = dot_nt(jnp.concatenate(lhs, -1), jnp.concatenate([wc2[base], wc2[base + 1]], -1))
                    acc = term if acc is None else acc + term
                parts.append(acc.reshape(many, triples, TRIPLE, c2))
            every.append(parts)
        history(
            count, second, third, up2, down2, side_a, side_b, dau, dbu, dad, dbd, w2, w3c,
            part2, part3, e_lo, e_hi, e3, xc2, xc3,
        )
        for q in range(2):
            parts = every[q]
            top_edge = within & ((row > 0) | lower | (spot < flags[0] * TRIPLE))
            bottom_edge = within & ((row < 2) | ~lower | (spot < flags[1] * TRIPLE))
            for f in range(frames):
                for i in range(triples):
                    value = parts[2][f, i]
                    if f >= 1:
                        value = value + parts[1][f - 1, i]
                    if f >= 2:
                        value = value + parts[0][f - 2, i]
                    else:
                        value = value + part2[q, f, i]
                    keep = top_edge if i == 0 else bottom_edge if i == triples - 1 else within
                    value = jnp.where(keep, value.astype(BF16).astype(F32), 0.0)
                    square = value * value
                    sum_low = jnp.sum(jnp.where(lower, square, 0.0), axis=-1, keepdims=True)
                    sum_high = jnp.sum(jnp.where(lower, 0.0, square), axis=-1, keepdims=True)
                    scale = jnp.where(
                        lower,
                        lax.rsqrt(sum_low * (1.0 / c3) + EPS),
                        lax.rsqrt(sum_high * (1.0 / c3) + EPS),
                    )
                    value = value * scale * gain
                    value = value / (1.0 + jnp.exp(-value))
                    for j in range(3):
                        e2[f, 3 * i + j, off:off + ringed, 0:c2] = value[j * ringed:(j + 1) * ringed]
            for f in range(frames):
                for r in range(rows2):
                    for cs in ((1, 3) if q == 0 else (0, 2)):
                        start = off + (0, 1, 1, 2)[cs]
                        x3[cs, f, r] = e2[f, r, start:start + width, :].astype(BF16)

    @pl.when(always)
    def _():
        acc = None
        for rs in range(2):
            for cs in (0, 2):
                lhs = [
                    x3[i, :, rs:rs + height].reshape(frames * height * width, lanes2) for i in (cs, cs + 1)
                ]
                base = (rs * 4 + cs) * 192
                rhs = [wc3[base:base + 192], wc3[base + 192:base + 384]]
                term = dot_nt(jnp.concatenate(lhs, -1), jnp.concatenate(rhs, -1))
                acc = term if acc is None else acc + term
        size = height * width
        acc = acc.reshape(frames, size, 192)
        turned = []
        for f in range(frames):
            value = acc[f, :, 0:64]
            if f >= 1:
                value = value + acc[f - 1, :, 64:128]
            value = value + (acc[f - 2, :, 128:192] if f >= 2 else part3[f])
            value = value.T
            turned.append(jnp.concatenate([value[b * 16:(b + 1) * 16] for b in range(4)], -1))
        turned = jnp.concatenate(turned, 0)
        row = lax.broadcasted_iota(jnp.int32, (4 * size, 4 * size), 0)
        lane = lax.broadcasted_iota(jnp.int32, (4 * size, 4 * size), 1)
        place = row % size * 4 + row // size
        spread = jnp.where(place == lane, 1.0, 0.0).astype(BF16)
        result = None
        for _ in range(3):
            piece = turned.astype(BF16)
            turned = turned - piece.astype(F32)
            term = jnp.dot(piece, spread, preferred_element_type=F32)
            result = term if result is None else result + term
        for f in range(frames):
            for c in range(out.shape[1]):
                for r in range(height):
                    out[f, c, 4 * r:4 * r + 4, :] = result[
                        f * 16 + c * 4:f * 16 + c * 4 + 4, r * 4 * width:(r + 1) * 4 * width
                    ]


def body(count, features, cache_first, cache_second, cache_third, w1, w2, w3, g1, g2, g3):
    tile_rows = count // TILES_X
    last_dims = lambda v: v[:, :, 0].transpose(0, 2, 3, 1)
    feats, old1, old2, old3 = map(last_dims, (features, cache_first, cache_second, cache_third))
    frames, height, width, c1 = feats.shape
    old = old1.shape[0]
    total = frames + old
    c2, c3 = old2.shape[-1], old3.shape[-1]
    rgb = w3.shape[3]
    row_pairs = [0] if tile_rows <= 2 else [0, 1]
    vmem = pl.BlockSpec(memory_space=pltpu.VMEM)
    bf = lambda *shape: jax.ShapeDtypeStruct(shape, BF16)

    def call(kernel, ins, outs, scratch, limit, flops, far=()):
        fn = pl.pallas_call(
            kernel,
            out_shape=outs,
            in_specs=[pl.BlockSpec(memory_space=pltpu.HBM) if i in far else vmem for i in range(len(ins))],
            out_specs=[vmem] * len(outs),
            scratch_shapes=scratch,
            compiler_params=pltpu.CompilerParams(vmem_limit_bytes=int(limit * 2**20)),
            cost_estimate=pl.CostEstimate(flops=flops, bytes_accessed=2_000_000, transcendentals=0),
        )
        ins = [pltpu.with_memory_space_constraint(v, pltpu.HBM) if i in far else v for i, v in enumerate(ins)]
        return fn(*ins)

    side = bf(total * height + old * 2 * height, 2, c1)
    corner = bf(total * 2 + old * 2, 2, c1)
    rows = [bf(old, 2, 2 * width, c1), bf(total, 2, width, c1)]
    packed = call(
        functools.partial(pack_kernel, count, row_pairs), (feats, old1, old2, old3),
        [side] * 2 + (rows + [corner] * 2) * len(row_pairs),
        [
            pltpu.VMEM(feats.shape, BF16),
            pltpu.VMEM(old1.shape, BF16),
            pltpu.VMEM(old2.shape, BF16),
            pltpu.VMEM((old, 2, 4 * width, c3), BF16),
            pltpu.VMEM((old, 4 * height, 8, c3), BF16),
            pltpu.VMEM((old, 4 * height, 8, c3), BF16),
            pltpu.SemaphoreType.DMA((7,)),
        ],
        8, 100_000_000, range(4),
    )

    sent = [swap(packed[cp], count, None, cp) for cp in (0, 1)]
    rows1, rows2, corners = [], [], ([], [])
    for i, rp in enumerate(row_pairs):
        piece = packed[2 + 4 * i:6 + 4 * i]
        rows2.append(swap(piece[0], count, rp, None))
        for cp in (0, 1):
            corners[cp].append(swap(piece[2 + cp], count, rp, cp))
        rows1.append(swap(piece[1], count, rp, None))
    odd_row = (lax.axis_index("tile") + TILES_X // 2) // TILES_X % 2 == 1

    def above(pieces):
        return pieces[0] if len(pieces) == 1 else jnp.where(odd_row, pieces[0], pieces[1])

    def below(pieces):
        return pieces[0] if len(pieces) == 1 else jnp.where(odd_row, pieces[1], pieces[0])

    diagonals = [pick(corners[cp]) for pick in (above, below) for cp in (0, 1)]
    size = height * width
    w1, w2, wc2, wc3, w3c = call(
        weights_kernel, (w1, w2, w3),
        [bf(*w1.shape), bf(*w2.shape), bf(24, 2 * c3, 256), bf(8 * 192, 256), bf(36 * 128, 128)],
        [pltpu.VMEM((128, 128), F32), pltpu.SemaphoreType.DMA((2,))], 16, 500_000_000, (0, 1),
    )
    (x2,) = call(
        functools.partial(first_kernel, count),
        (feats, old1, above(rows1), below(rows1), *sent, *diagonals, w1, g1, g2),
        [bf(3, frames, 2, (height + 1) // 3, TRIPLE, 256)],
        [
            pltpu.VMEM((total, height + 4, 40, c1), F32),
            pltpu.VMEM((3, total, 2, height // 2 + 2, PAIR, c1), BF16),
            pltpu.VMEM((frames, height + 2, 40, 256), F32),
        ],
        22, 6_000_000_000,
    )
    (out,) = call(
        functools.partial(last_kernel, count),
        (old2, old3, above(rows2), below(rows2), *sent, *diagonals, w2, w3c, x2, g3, wc2, wc3),
        [jax.ShapeDtypeStruct((frames, rgb, 4 * height, 4 * width), F32)],
        [
            pltpu.VMEM((2, 2, (height + 1) // 3, TRIPLE, c2), F32),
            pltpu.VMEM((2, size, 64), F32),
            pltpu.VMEM((old, 2 * height + 4, 64, 128), F32),
            pltpu.VMEM((old, 2 * height + 4, 64, 128), F32),
            pltpu.VMEM((old, 4 * height + 2, 96, 128), F32),
            pltpu.VMEM((4, old, 2 * height + 4, PITCH, c2), BF16),
            pltpu.VMEM((6, old, height + 1, 4, width, 128), BF16),
            pltpu.VMEM((frames, height + 2, 40, 256), F32),
            pltpu.VMEM((4, frames, height + 1, width, 256), BF16),
        ],
        30, 8_000_000_000,
    )
    return out[:, :, None]


def solution(mesh):
    tiled = P("groups", None, "tile", None, None)
    return jax.shard_map(
        functools.partial(body, mesh.shape["tile"]),
        mesh=mesh,
        in_specs=(tiled,) * 4 + (P(),) * 6,
        out_specs=tiled,
        check_vma=False,
    )
```
